32 devices in a mesh: row: 4 (over x, core), col: 8 (over z, y).
Axes of the slice: x: 2, y: 2, z: 4, core: 2. Of those that a mesh axis runs over, the one named last changes fastest.
Arguments:
- swath: int32 [640, 4096], P('row', 'col'), may hold values from 0 to 1
- coherence: int32 [640, 4096], P('row', 'col'), may hold values from 0 to 7
- phase_counts: int32 [640, 4096], P('row', 'col'), may hold values from 0 to 255
Outputs:
- unwrapped: float32 [640, 4096], P('row', 'col')
The draws below stay inside these ranges and needn't reach their ends.
All inputs are finite; a program needn't handle non-finite values.
Results may differ from the reference program's by a relative error of at most 0.0012.
Values sent between devices are 32-bit elements; how exact they have to be, the bound alone decides.
No kernel may reach another device: no remote copies, remote signals or barrier semaphores. Data moves between devices by JAX's collectives and lax.ppermute only.
A program may use at most 128 MiB of HBM per device.

```python
import jax
import jax.numpy as jnp
from jax import lax

GRIDS = 4
LEVELS = 256
NCLASS = 8
NX = 640
NY = 4096


def draw_swath(key, part):
    rows = jnp.arange(NX, dtype=jnp.int32)[:, None]
    columns = jnp.arange(NY, dtype=jnp.int32)[None, :]
    threshold = 300 + 325 * rows // NX + 325 * columns // NY
    sample = jax.random.randint(jax.random.fold_in(key, 11), (NX, NY), 0, 1000, dtype=jnp.int32)
    return (sample < threshold).astype(jnp.int32)


def with_ends(array, rng, low, high):
    longest = array.shape.index(max(array.shape))
    spots = []
    for shift in (0, 1):
        where = [jax.random.randint(jax.random.fold_in(rng, axis), (), 0, length) for axis, length in enumerate(array.shape)]
        where[longest] = (where[longest] + shift) % array.shape[longest]
        spots.append(tuple(where))
    return array.at[spots[0]].set(low).at[spots[1]].set(high)


def setup_inputs(seed: int = 0) -> dict:
    seeds = jax.random.split(jax.random.key(seed), 4)
    swath = draw_swath(jax.random.fold_in(seeds[3], 71), 0)
    coherence = with_ends(jax.random.randint(seeds[1], (NX, NY), 0, NCLASS), jax.random.fold_in(seeds[1], 1), 0, NCLASS - 1).astype(jnp.int32)
    phase_counts = with_ends(jax.random.randint(seeds[2], (NX, NY), 0, LEVELS), jax.random.fold_in(seeds[2], 1), 0, LEVELS - 1).astype(jnp.int32)
    return dict(swath=swath, coherence=coherence, phase_counts=phase_counts)


damping = 0.8
diag_floor = 0.5
error_floor = 0.5
epsilon = 1e-06
screen_width = 4.0
highest = lax.Precision.HIGHEST

def cosine_table(count):
    freq = jnp.arange(count, dtype=jnp.float32)[:, None]
    place = jnp.arange(count, dtype=jnp.float32)[None, :]
    table = jnp.cos(jnp.pi * (place + 0.5) * freq / count) * jnp.sqrt(2.0 / count)
    return jnp.where(freq == 0, table * jnp.sqrt(0.5), table)

def eigen_values(freq, count):
    return 2.0 - 2.0 * jnp.cos(jnp.pi * freq / count)

def weight_diagonal(w_down, w_right):
    w_up = jnp.pad(w_down, ((1, 0), (0, 0)))[:-1]
    w_left = jnp.pad(w_right, ((0, 0), (1, 0)))[:, :-1]
    return w_down + w_up + w_right + w_left

def operate(estimate, w_down, w_right, diagonal):
    padded = jnp.pad(estimate, 1)
    w_up = jnp.pad(w_down, ((1, 0), (0, 0)))[:-1]
    w_left = jnp.pad(w_right, ((0, 0), (1, 0)))[:, :-1]
    beside = w_down * padded[2:, 1:-1] + w_up * padded[:-2, 1:-1] + w_right * padded[1:-1, 2:] + w_left * padded[1:-1, :-2]
    return diagonal * estimate - beside

def coarse_solve(source, w_down, w_right):
    rows, cols = source.shape
    count = (rows - 1) * cols + rows * (cols - 1)
    mean = (jnp.sum(w_down) + jnp.sum(w_right)) / count + epsilon
    table_x = cosine_table(rows)
    table_y = cosine_table(cols)
    spectrum = jnp.dot(jnp.dot(table_x, source, precision=highest), table_y.T, precision=highest)
    lam_x = eigen_values(jnp.arange(rows, dtype=jnp.float32), rows)
    lam_y = eigen_values(jnp.arange(cols, dtype=jnp.float32), cols)
    spectrum = spectrum / (mean * (lam_x[:, None] + lam_y[None, :] + (screen_width / cols) ** 2))
    return jnp.dot(table_x.T, jnp.dot(spectrum, table_y, precision=highest), precision=highest)

def cycle(estimate, source, w_down, w_right, depth):
    if depth == GRIDS:
        return coarse_solve(source, w_down, w_right)
    diagonal = weight_diagonal(w_down, w_right)
    divisor = jnp.maximum(diagonal, diag_floor)
    estimate = estimate + damping * (source - operate(estimate, w_down, w_right, diagonal)) / divisor
    residual = source - operate(estimate, w_down, w_right, diagonal)
    rows, cols = residual.shape
    coarse_source = residual.reshape(rows // 2, 2, cols // 2, 2).sum(axis=(1, 3))
    coarse_down = w_down[1::2, 0::2] + w_down[1::2, 1::2]
    coarse_right = w_right[0::2, 1::2] + w_right[1::2, 1::2]
    correction = cycle(jnp.zeros_like(coarse_source), coarse_source, coarse_down, coarse_right, depth + 1)
    estimate = estimate + jnp.repeat(jnp.repeat(correction, 2, axis=0), 2, axis=1)
    return estimate + damping * (source - operate(estimate, w_down, w_right, diagonal)) / divisor

def build_source(w_down, w_right, slope_down, slope_right):
    flux_down = w_down * slope_down
    flux_right = w_right * slope_right
    flux_up = jnp.pad(flux_down, ((1, 0), (0, 0)))[:-1]
    flux_left = jnp.pad(flux_right, ((0, 0), (1, 0)))[:, :-1]
    return flux_up - flux_down + flux_left - flux_right

def reference(swath, coherence, phase_counts):
    quality = swath.astype(jnp.float32) * (coherence.astype(jnp.float32) / (NCLASS - 1)) ** 2
    zero_row = jnp.zeros((1, NY), jnp.float32)
    zero_column = jnp.zeros((NX, 1), jnp.float32)
    w_down = jnp.concatenate([jnp.minimum(quality[:-1], quality[1:]), zero_row], 0)
    w_right = jnp.concatenate([jnp.minimum(quality[:, :-1], quality[:, 1:]), zero_column], 1)
    half = LEVELS // 2
    turn = 2.0 * jnp.pi / LEVELS
    step_down = jnp.mod(phase_counts[1:] - phase_counts[:-1] + half, LEVELS) - half
    step_right = jnp.mod(phase_counts[:, 1:] - phase_counts[:, :-1] + half, LEVELS) - half
    slope_down = jnp.concatenate([step_down.astype(jnp.float32) * turn, zero_row], 0)
    slope_right = jnp.concatenate([step_right.astype(jnp.float32) * turn, zero_column], 1)
    source = build_source(w_down, w_right, slope_down, slope_right)
    first = cycle(jnp.zeros((NX, NY), jnp.float32), source, w_down, w_right, 0)
    padded = jnp.pad(first, 1)
    error_down = padded[2:, 1:-1] - first - slope_down
    error_right = padded[1:-1, 2:] - first - slope_right
    reweighted_down = w_down / jnp.maximum(jnp.abs(error_down), error_floor)
    reweighted_right = w_right / jnp.maximum(jnp.abs(error_right), error_floor)
    source = build_source(reweighted_down, reweighted_right, slope_down, slope_right)
    return cycle(first, source, reweighted_down, reweighted_right, 0)
```

```python
import functools

import jax
import jax.numpy as jnp
import numpy as np
from jax import lax
from jax.experimental import pallas as pl
from jax.experimental.pallas import tpu as pltpu
from jax.sharding import PartitionSpec as P

GRIDS = 4
LEVELS = 256
NCLASS = 8

damping = 0.8
diag_floor = 0.5
error_floor = 0.5
epsilon = 1e-06
screen_width = 4.0
highest = lax.Precision.HIGHEST

CELL = 2**GRIDS
ROW_HALO = 3 * CELL
COL_HALO = 64
SUB = 8
LANE = 128


class Shape:
    def __init__(self, rows, cols, row_count, col_count):
        self.rows, self.cols = rows, cols
        self.row_count, self.col_count = row_count, col_count
        unit = SUB * CELL
        self.ext_rows = -(-(rows + 2 * ROW_HALO) // unit) * unit
        self.lanes = cols + 2 * COL_HALO
        self.chunk = self.ext_rows // SUB
        self.tiles = cols // LANE
        self.crows, self.ccols = rows // CELL, cols // CELL
        self.per_chunk = self.chunk // CELL
        self.grid_rows = self.crows * row_count
        self.grid_cols = self.ccols * col_count

    def slabs(self, depth):
        return self.chunk >> depth


def quality_of(swath, coherence):
    scaled = coherence.astype(jnp.float32) / (NCLASS - 1)
    return swath.astype(jnp.float32) * (scaled * scaled)


def lane_index(width):
    return lax.broadcasted_iota(jnp.int32, (SUB, width), 1)


def right_of(x, steps):
    return pltpu.roll(x, x.shape[1] - steps, 1)


def left_of(x, steps):
    return pltpu.roll(x, steps, 1)


def chunk_below(x):
    return pltpu.roll(x, SUB - 1, 0)


def chunk_above(x):
    return pltpu.roll(x, 1, 0)


def wrap_steps(difference):
    turns = jnp.floor(difference * (1.0 / LEVELS) + 0.5)
    return (difference - LEVELS * turns) * (2.0 * jnp.pi / LEVELS)


def relax_weight(diagonal):
    return damping / jnp.maximum(diagonal, diag_floor)


def row_strip_kernel(swath, coherence, counts, top, bottom):
    rows = swath.shape[0]
    for start, out in ((0, top), (rows - ROW_HALO, bottom)):
        here = slice(start, start + ROW_HALO)
        out[0:ROW_HALO, :] = quality_of(swath[here, :], coherence[here, :])
        out[ROW_HALO : 2 * ROW_HALO, :] = counts[here, :].astype(jnp.float32)


def col_strip_kernel(swath, coherence, counts, above, below, first, last, *, shape):
    rows, cols, ext = shape.rows, shape.cols, shape.ext_rows
    low = lax.broadcasted_iota(jnp.int32, (1, LANE), 1) < COL_HALO

    def put(where, quality, phase):
        first[where, :] = jnp.where(low, quality[0], pltpu.roll(phase[0], COL_HALO, 1))
        last[where, :] = jnp.where(low, pltpu.roll(phase[1], COL_HALO, 1), quality[1])

    sides = (slice(0, LANE), slice(cols - LANE, cols))
    put(
        slice(0, rows),
        [quality_of(swath[:, s], coherence[:, s]) for s in sides],
        [counts[:, s].astype(jnp.float32) for s in sides],
    )
    for ref, start in ((below, rows), (above, ext - ROW_HALO)):
        put(
            slice(start, start + ROW_HALO),
            [ref[0:ROW_HALO, s] for s in sides],
            [ref[ROW_HALO : 2 * ROW_HALO, s] for s in sides],
        )
    if ext > rows + 2 * ROW_HALO:
        gap = slice(rows + ROW_HALO, ext - ROW_HALO)
        first[gap, :] = jnp.zeros_like(first[gap, :])
        last[gap, :] = jnp.zeros_like(last[gap, :])


def pair_sum(x, steps, odd):
    y = x + right_of(x, steps)
    return jnp.where(odd, left_of(y, steps), y)


def odd_value(x, steps, odd):
    return jnp.where(odd, x, right_of(x, steps))


def go_down(fine, coarse, depth, shape):
    steps = 1 << depth
    count = shape.slabs(depth + 1)
    odd = (lane_index(shape.lanes) & steps) != 0
    a_f, b_f, gd_f, gr_f, v_f = (fine[k] for k in ("a", "b", "gd", "gr", "est"))
    last_level = depth + 1 == GRIDS
    wrapped = chunk_below(v_f[0])

    def down_part(k, v_next):
        a = a_f[2 * k + 1]
        flux = gd_f[2 * k + 1] + a * (v_next - v_f[2 * k + 1])
        return pair_sum(a, steps, odd), pair_sum(flux, steps, odd)

    def step(k, v_next, a_prev, gd_prev):
        a, gd = down_part(k, v_next)
        v0, v1 = v_f[2 * k], v_f[2 * k + 1]
        b0, b1 = b_f[2 * k], b_f[2 * k + 1]
        fr = gr_f[2 * k] + gr_f[2 * k + 1] + b0 * (right_of(v0, steps) - v0) + b1 * (right_of(v1, steps) - v1)
        b = odd_value(b0 + b1, steps, odd)
        gr = odd_value(fr, steps, odd)
        right_side = gd - gd_prev + gr - left_of(gr, 2 * steps)
        if last_level:
            coarse["w"][k] = a + b
            coarse["est"][k] = right_side
        else:
            w = relax_weight(a + a_prev + b + left_of(b, 2 * steps))
            coarse["a"][k] = a
            coarse["b"][k] = b
            coarse["gd"][k] = gd
            coarse["gr"][k] = gr
            coarse["w"][k] = w
            coarse["est"][k] = w * right_side
        return a, gd

    a, gd = down_part(count - 1, wrapped)
    carry = (chunk_above(a), chunk_above(gd))
    carry = lax.fori_loop(0, count - 1, lambda k, c: step(k, v_f[2 * k + 2], *c), carry)
    step(count - 1, wrapped, *carry)


def lane_select(shape):
    place = lax.broadcasted_iota(jnp.int32, (shape.cols, LANE), 0)
    target = lax.broadcasted_iota(jnp.int32, (shape.cols, LANE), 1)
    return (place == target * CELL).astype(jnp.bfloat16)


def three_parts(x):
    high = x.astype(jnp.bfloat16)
    rest = x - high.astype(jnp.float32)
    middle = rest.astype(jnp.bfloat16)
    low = (rest - middle.astype(jnp.float32)).astype(jnp.bfloat16)
    return high, middle, low


def select_product(x, one_hot):
    n = x.shape[0]
    parts = jnp.concatenate(list(three_parts(x)), axis=0)
    out = jnp.dot(parts, one_hot, preferred_element_type=jnp.float32)
    return out[0:n] + out[n : 2 * n] + out[2 * n : 3 * n]


def publish(coarse, out, shape):
    per = shape.per_chunk
    weights = sum(coarse["w"][j][:, : shape.cols] for j in range(per))
    fields = [coarse["est"][j][:, : shape.cols] for j in range(per)] + [weights]
    packed = select_product(jnp.concatenate(fields, axis=0), lane_select(shape))
    block = packed[0:SUB]
    for j in range(1, per + 1):
        block = block + pltpu.roll(packed[j * SUB : (j + 1) * SUB], j * shape.ccols, 1)
    for device in range(shape.row_count * shape.col_count):
        out[device] = block


LEVEL_KEYS = ("a", "b", "gd", "gr", "w", "est")


def levels_down(level0, levels, last, out, shape):
    chain = [level0] + levels + [last]
    for depth in range(GRIDS):
        go_down(chain[depth], chain[depth + 1], depth, shape)
    publish(last, out, shape)


def coarse_correction(gathered, table, shape, corr):
    rows, cols = shape.row_count, shape.col_count
    per, crows, ccols = shape.per_chunk, shape.crows, shape.ccols
    gr, gc = shape.grid_rows, shape.grid_cols
    group = LANE // ccols
    lane = lane_index(LANE)
    blocks = []
    for j in range(per):
        for r in range(rows):
            pieces = []
            for tile in range(cols // group):
                piece = None
                for g in range(group):
                    x = gathered[r * cols + tile * group + g]
                    shift = ((g - j) * ccols) % LANE
                    x = pltpu.roll(x, shift, 1) if shift else x
                    piece = x if piece is None else jnp.where(lane >= g * ccols, x, piece)
                pieces.append(piece)
            blocks.append(jnp.concatenate(pieces, axis=1))
    strip = jnp.concatenate(blocks, axis=0)

    weights = gathered[0]
    for device in range(1, rows * cols):
        weights = weights + gathered[device]
    sub = lax.broadcasted_iota(jnp.int32, (SUB, LANE), 0)
    own = (sub < crows // per) & (lane >= per * ccols) & (lane < (per + 1) * ccols)
    total = jnp.sum(jnp.where(own, weights, 0.0), keepdims=True)
    count = (gr - 1) * gc + gr * (gc - 1)
    mean = total / count + epsilon

    def at(dim, size):
        return lax.broadcasted_iota(jnp.int32, size, dim)

    def cosines(freq, place):
        value = jnp.cos((jnp.pi / gr) * ((place.astype(jnp.float32) + 0.5) * freq.astype(jnp.float32)))
        return jnp.where(freq == 0, np.float32(np.sqrt(1.0 / gr)), np.float32(np.sqrt(2.0 / gr)) * value)

    size = (gr, per * rows * SUB)
    column = at(1, size)
    chunk = column % SUB
    place = (column // SUB) % rows * crows + chunk * per + column // (SUB * rows)
    inside = chunk < crows // per
    forward_x = jnp.where(inside, cosines(at(0, size), jnp.where(inside, place, 0)), 0.0)

    size = (per * SUB, gr)
    slot = (at(0, size) % SUB) * per + at(0, size) // SUB
    slots = SUB * per
    local = jnp.where(slot < slots - ROW_HALO // CELL, slot, slot - slots)
    backward_x = cosines(at(1, size), lax.axis_index("row") * crows + local)

    spectrum = lax.dot_general(strip, table[...], (((1,), (1,)), ((), ())), precision=highest)
    spectrum = jnp.dot(forward_x, spectrum, precision=highest)
    size = (gr, gc)

    def eigen(index, n):
        return 2.0 - 2.0 * jnp.cos((jnp.pi / n) * index.astype(jnp.float32))

    lam = eigen(at(0, (gr, 1)), gr) + eigen(at(1, (1, gc)), gc)
    screen = (screen_width / gc) ** 2
    spectrum = spectrum / (mean * (lam + screen))
    values = jnp.dot(backward_x, spectrum, precision=highest)
    values = jnp.dot(values, table[...], precision=highest)

    size = (gc, shape.lanes)
    cell = at(1, size) // CELL
    edge = (shape.cols + COL_HALO) // CELL
    cell = jnp.where(cell < edge, cell, cell - shape.lanes // CELL)
    spread = (at(0, size) == cell + lax.axis_index("col") * ccols).astype(jnp.bfloat16)
    values = select_product(values, spread)
    for j in range(per):
        corr[j] = values[j * SUB : (j + 1) * SUB]


def go_up(level, corr, depth, shape, emit):
    steps = 1 << depth
    count = shape.slabs(depth)
    a_r, b_r, gd_r, gr_r, w_r, e_r = (level[k] for k in LEVEL_KEYS)

    def down_flux(i, v, v_next):
        return gd_r[i] + a_r[i] * (v_next - v)

    def sweep(i, v, v_next, f_prev):
        fd = down_flux(i, v, v_next)
        fr = gr_r[i] + b_r[i] * (right_of(v, steps) - v)
        emit(i, v + w_r[i] * (fd - f_prev + fr - left_of(fr, steps)))
        return fd

    def pair(k, v0, v2, f_prev):
        v1 = e_r[2 * k + 1] + corr[k]
        f_prev = sweep(2 * k, v0, v1, f_prev)
        return sweep(2 * k + 1, v1, v2, f_prev)

    v_first = e_r[0] + corr[0]
    wrapped = chunk_below(v_first)
    v_last = e_r[count - 1] + corr[count // 2 - 1]
    f_prev = chunk_above(down_flux(count - 1, v_last, wrapped))

    def body(k, carry):
        v0, f_prev = carry
        v2 = e_r[2 * k + 2] + corr[k + 1]
        return v2, pair(k, v0, v2, f_prev)

    v0, f_prev = lax.fori_loop(0, count // 2 - 1, body, (v_first, f_prev))
    pair(count // 2 - 1, v0, wrapped, f_prev)


def levels_up(levels, corr, results, shape):
    for depth in range(GRIDS - 1, 0, -1):
        out = results[depth - 1]

        def emit(i, value, out=out):
            out[i] = value

        go_up(levels[depth - 1], corr, depth, shape, emit)
        corr = out
    return corr


def as_levels(refs):
    n = len(LEVEL_KEYS)
    return [dict(zip(LEVEL_KEYS, refs[i : i + n])) for i in range(0, len(refs), n)]


def start_kernel(*refs, shape):
    (swath, coherence, counts, above, below, from_right, from_left) = refs[:7]
    out = refs[7]
    sd_r, sr_r = refs[8:10]
    level_refs = refs[10 : 10 + 6 * GRIDS]
    nat_q, nat_n, rhs, wsum = refs[10 + 6 * GRIDS :]
    rows, ext, tiles = shape.rows, shape.ext_rows, shape.tiles
    level0, *levels = as_levels(level_refs)
    last = dict(est=rhs, w=wsum)

    for t in range(tiles):
        lanes = slice(t * LANE, (t + 1) * LANE)
        nat_q[t, 0:rows, :] = quality_of(swath[:, lanes], coherence[:, lanes])
        nat_n[t, 0:rows, :] = counts[:, lanes].astype(jnp.float32)
        for ref, start in ((below, rows), (above, ext - ROW_HALO)):
            nat_q[t, start : start + ROW_HALO, :] = ref[0:ROW_HALO, lanes]
            nat_n[t, start : start + ROW_HALO, :] = ref[ROW_HALO : 2 * ROW_HALO, lanes]
        if ext > rows + 2 * ROW_HALO:
            gap = slice(rows + ROW_HALO, ext - ROW_HALO)
            nat_q[t, gap, :] = jnp.zeros_like(nat_q[t, gap, :])
            nat_n[t, gap, :] = jnp.zeros_like(nat_n[t, gap, :])
    low = lane_index(LANE) < COL_HALO

    def load(i):
        rows_of = pl.ds(i, SUB, stride=shape.chunk)
        right, left = from_right[rows_of, :], from_left[rows_of, :]
        quality = [nat_q[t, rows_of, :] for t in range(tiles)] + [jnp.where(low, right, left)]
        phase = [nat_n[t, rows_of, :] for t in range(tiles)]
        phase += [pltpu.roll(jnp.where(low, left, right), COL_HALO, 1)]
        return jnp.concatenate(quality, axis=1), jnp.concatenate(phase, axis=1)

    count = shape.chunk

    def down_part(q, n, q_next, n_next):
        a = jnp.minimum(q, q_next)
        sd = wrap_steps(n_next - n)
        return a, sd, -(a * sd)

    def step(i, q, n, q_next, n_next, a_prev, gd_prev):
        a, sd, gd = down_part(q, n, q_next, n_next)
        b = jnp.minimum(q, right_of(q, 1))
        sr = wrap_steps(right_of(n, 1) - n)
        gr = -(b * sr)
        w = relax_weight(a + a_prev + b + left_of(b, 1))
        level0["a"][i] = a
        level0["b"][i] = b
        level0["gd"][i] = gd
        level0["gr"][i] = gr
        level0["w"][i] = w
        level0["est"][i] = w * (gd - gd_prev + gr - left_of(gr, 1))
        sd_r[i] = sd
        sr_r[i] = sr
        return a, gd

    q0, n0 = load(0)
    q_wrap, n_wrap = chunk_below(q0), chunk_below(n0)
    a, _, gd = down_part(*load(count - 1), q_wrap, n_wrap)

    def body(i, carry):
        q, n, a, gd = carry
        q_next, n_next = load(i + 1)
        a, gd = step(i, q, n, q_next, n_next, a, gd)
        return q_next, n_next, a, gd

    q, n, a, gd = lax.fori_loop(0, count - 1, body, (q0, n0, chunk_above(a), chunk_above(gd)))
    step(count - 1, q, n, q_wrap, n_wrap, a, gd)
    levels_down(level0, levels, last, out, shape)


def middle_kernel(*refs, shape):
    gathered, table, sd_r, sr_r = refs[:4]
    old = as_levels(refs[4 : 4 + 6 * GRIDS])
    refs = refs[4 + 6 * GRIDS :]
    out, first = refs[:2]
    level0, *levels = as_levels(refs[2 : 2 + 6 * GRIDS])
    rhs, wsum, corr, *results = refs[2 + 6 * GRIDS :]
    coarse_correction(gathered, table, shape, corr)
    field = levels_up(old[1:], corr, results, shape)

    def emit(i, value):
        first[i] = value

    go_up(old[0], field, 0, shape, emit)

    count = shape.chunk
    a_old, b_old = old[0]["a"], old[0]["b"]

    def down_part(i, v, v_next):
        error = v_next - v - sd_r[i]
        a = a_old[i] / jnp.maximum(jnp.abs(error), error_floor)
        return a, a * error

    def step(i, v, v_next, a_prev, gd_prev):
        a, gd = down_part(i, v, v_next)
        error = right_of(v, 1) - v - sr_r[i]
        b = b_old[i] / jnp.maximum(jnp.abs(error), error_floor)
        gr = b * error
        w = relax_weight(a + a_prev + b + left_of(b, 1))
        level0["a"][i] = a
        level0["b"][i] = b
        level0["gd"][i] = gd
        level0["gr"][i] = gr
        level0["w"][i] = w
        level0["est"][i] = w * (gd - gd_prev + gr - left_of(gr, 1))
        return a, gd

    wrapped = chunk_below(first[0])
    a, gd = down_part(count - 1, first[count - 1], wrapped)

    def body(i, carry):
        v, a, gd = carry
        v_next = first[i + 1]
        return v_next, *step(i, v, v_next, a, gd)

    v, a, gd = lax.fori_loop(0, count - 1, body, (first[0], chunk_above(a), chunk_above(gd)))
    step(count - 1, v, wrapped, a, gd)
    levels_down(level0, levels, dict(est=rhs, w=wsum), out, shape)


def end_kernel(*refs, shape):
    gathered, table, first = refs[:3]
    old = as_levels(refs[3 : 3 + 6 * GRIDS])
    out, nat, corr, *results = refs[3 + 6 * GRIDS :]
    coarse_correction(gathered, table, shape, corr)
    field = levels_up(old[1:], corr, results, shape)

    def emit(i, value):
        value = value + first[i]
        for t in range(shape.tiles):
            nat[t, pl.ds(i, SUB, stride=shape.chunk), :] = value[:, t * LANE : (t + 1) * LANE]

    go_up(old[0], field, 0, shape, emit)
    for t in range(shape.tiles):
        out[:, t * LANE : (t + 1) * LANE] = nat[t, 0 : shape.rows, :]


def dct_table(count):
    freq = np.arange(count)[:, None]
    place = np.arange(count)[None, :]
    table = np.cos(np.pi * (((2 * place + 1) * freq) % (4 * count)) / (2 * count)) * np.sqrt(2.0 / count)
    table[0] *= np.sqrt(0.5)
    return table.astype(np.float32)


def f32(*dims):
    return jax.ShapeDtypeStruct(dims, jnp.float32)


def level_shapes(shape):
    return [f32(shape.slabs(d), SUB, shape.lanes) for d in range(GRIDS) for _ in LEVEL_KEYS]


def vmem(*dims):
    return pltpu.VMEM(dims, jnp.float32)


def exchange(lower, upper, axis):
    count = lax.axis_size(axis)
    up = [(i, i + 1) for i in range(count - 1)]
    down = [(i + 1, i) for i in range(count - 1)]
    return lax.ppermute(upper, axis, up), lax.ppermute(lower, axis, down)


def body(swath, coherence, phase_counts, *, shape):
    params = pltpu.CompilerParams(vmem_limit_bytes=40 * 2**20)
    inputs = (swath, coherence, phase_counts)
    devices = shape.row_count * shape.col_count
    block = f32(devices, SUB, LANE)
    table = jnp.asarray(dct_table(shape.grid_cols))
    coarse_scratch = [vmem(shape.per_chunk, SUB, shape.lanes)] * 2
    result_scratch = [vmem(shape.per_chunk, SUB, shape.lanes)]
    result_scratch += [vmem(shape.slabs(d), SUB, shape.lanes) for d in range(1, GRIDS)]

    strip = f32(2 * ROW_HALO, shape.cols)
    top, bottom = pl.pallas_call(
        row_strip_kernel, out_shape=[strip, strip], compiler_params=params, name="row_strips"
    )(*inputs)
    above, below = exchange(top, bottom, "row")
    strip = f32(shape.ext_rows, LANE)
    first_cols, last_cols = pl.pallas_call(
        functools.partial(col_strip_kernel, shape=shape),
        out_shape=[strip, strip],
        compiler_params=params,
        name="col_strips",
    )(*inputs, above, below)
    from_left, from_right = exchange(first_cols, last_cols, "col")

    field = f32(shape.chunk, SUB, shape.lanes)
    nat = vmem(shape.tiles, shape.ext_rows, LANE)
    block_out, sd, sr, *old = pl.pallas_call(
        functools.partial(start_kernel, shape=shape),
        out_shape=[block, field, field] + level_shapes(shape),
        scratch_shapes=[nat, nat] + coarse_scratch,
        compiler_params=params,
        name="start",
    )(*inputs, above, below, from_right, from_left)
    gathered = lax.all_to_all(block_out, ("row", "col"), split_axis=0, concat_axis=0, tiled=True)
    block_out, first, *old = pl.pallas_call(
        functools.partial(middle_kernel, shape=shape),
        out_shape=[block, field] + level_shapes(shape),
        scratch_shapes=coarse_scratch + result_scratch,
        compiler_params=params,
        name="middle",
    )(gathered, table, sd, sr, *old)
    gathered = lax.all_to_all(block_out, ("row", "col"), split_axis=0, concat_axis=0, tiled=True)
    return pl.pallas_call(
        functools.partial(end_kernel, shape=shape),
        out_shape=f32(shape.rows, shape.cols),
        scratch_shapes=[nat] + result_scratch,
        compiler_params=params,
        name="finish",
    )(gathered, table, first, *old)


def solution(mesh):
    def run(swath, coherence, phase_counts):
        rows, cols = swath.shape
        row_count, col_count = mesh.shape["row"], mesh.shape["col"]
        shape = Shape(rows // row_count, cols // col_count, row_count, col_count)
        return jax.shard_map(
            functools.partial(body, shape=shape),
            mesh=mesh,
            in_specs=(P("row", "col"), P("row", "col"), P("row", "col")),
            out_specs=P("row", "col"),
            check_vma=False,
        )(swath, coherence, phase_counts)

    return run
```

```python
import functools

import jax
import jax.numpy as jnp
import numpy as np
from jax import lax
from jax.experimental import pallas as pl
from jax.experimental.pallas import tpu as pltpu
from jax.sharding import PartitionSpec as P

GRIDS = 4
LEVELS = 256
NCLASS = 8

damping = 0.8
diag_floor = 0.5
error_floor = 0.5
epsilon = 1e-06
screen_width = 4.0
highest = lax.Precision.HIGHEST

UNROLL = 4
WHOLE = 8

CELL = 2**GRIDS
ROW_HALO = 3 * CELL
COL_HALO = 64
SUB = 8
LANE = 128


class Shape:
    def __init__(self, rows, cols, row_count, col_count):
        self.rows, self.cols = rows, cols
        self.row_count, self.col_count = row_count, col_count
        unit = SUB * CELL
        self.ext_rows = -(-(rows + 2 * ROW_HALO) // unit) * unit
        self.lanes = cols + 2 * COL_HALO
        self.chunk = self.ext_rows // SUB
        self.tiles = cols // LANE
        self.crows, self.ccols = rows // CELL, cols // CELL
        self.per_chunk = self.chunk // CELL
        self.grid_rows = self.crows * row_count
        self.grid_cols = self.ccols * col_count

    def slabs(self, depth):
        return self.chunk >> depth


def quality_of(swath, coherence):
    scaled = coherence.astype(jnp.float32) / (NCLASS - 1)
    return swath.astype(jnp.float32) * (scaled * scaled)


def lane_index(width):
    return lax.broadcasted_iota(jnp.int32, (SUB, width), 1)


def right_of(x, steps):
    return pltpu.roll(x, x.shape[1] - steps, 1)


def left_of(x, steps):
    return pltpu.roll(x, steps, 1)


def chunk_below(x):
    return pltpu.roll(x, SUB - 1, 0)


def chunk_above(x):
    return pltpu.roll(x, 1, 0)


def wrap_steps(difference):
    turns = jnp.floor(difference * (1.0 / LEVELS) + 0.5)
    return (difference - LEVELS * turns) * (2.0 * jnp.pi / LEVELS)


def relax_weight(diagonal):
    return damping / jnp.maximum(diagonal, diag_floor)


def strips_kernel(swath, coherence, counts, quality, phase, top, bottom, s_buf, c_buf, p_buf, sems):
    rows = quality.shape[0]
    copies = [
        pltpu.make_async_copy(src, dst, sems.at[n])
        for n, (src, dst) in enumerate(((swath, s_buf), (coherence, c_buf), (counts, p_buf)))
    ]
    for copy in copies:
        copy.start()
    for copy in copies:
        copy.wait()
    for r in range(0, rows, 2 * SUB):
        here = slice(r, r + 2 * SUB)
        quality[here, :] = quality_of(s_buf[here, :], c_buf[here, :])
        phase[here, :] = p_buf[here, :].astype(jnp.float32)
    for start, out in ((0, top), (rows - ROW_HALO, bottom)):
        here = slice(start, start + ROW_HALO)
        out[0:ROW_HALO, :] = quality[here, :]
        out[ROW_HALO : 2 * ROW_HALO, :] = phase[here, :]


def col_strip_kernel(quality, phase, above, below, first, last, *, shape):
    rows, cols, ext = shape.rows, shape.cols, shape.ext_rows
    low = lax.broadcasted_iota(jnp.int32, (1, LANE), 1) < COL_HALO

    def put(where, q, n):
        first[where, :] = jnp.where(low, q[0], pltpu.roll(n[0], COL_HALO, 1))
        last[where, :] = jnp.where(low, pltpu.roll(n[1], COL_HALO, 1), q[1])

    sides = (slice(0, LANE), slice(cols - LANE, cols))
    put(
        slice(0, rows),
        [quality[:, s] for s in sides],
        [phase[:, s] for s in sides],
    )
    for ref, start in ((below, rows), (above, ext - ROW_HALO)):
        put(
            slice(start, start + ROW_HALO),
            [ref[0:ROW_HALO, s] for s in sides],
            [ref[ROW_HALO : 2 * ROW_HALO, s] for s in sides],
        )
    if ext > rows + 2 * ROW_HALO:
        gap = slice(rows + ROW_HALO, ext - ROW_HALO)
        first[gap, :] = jnp.zeros_like(first[gap, :])
        last[gap, :] = jnp.zeros_like(last[gap, :])


def run(count, step, carry):
    unroll = min(count, UNROLL)
    if count <= WHOLE:
        for i in range(count):
            carry = step(i, carry)
        return carry

    def turn(t, carry):
        for u in range(unroll):
            carry = step(t * unroll + u, carry)
        return carry

    carry = lax.fori_loop(0, count // unroll, turn, carry)
    for i in range(count // unroll * unroll, count):
        carry = step(i, carry)
    return carry


def close(field, count):
    field[count] = chunk_below(field[0])


def put_level(level, i, *values):
    for key, value in zip(LEVEL_KEYS, values):
        level[key][i] = value


def pair_sum(x, steps, odd):
    y = x + right_of(x, steps)
    return jnp.where(odd, left_of(y, steps), y)


def odd_value(x, steps, odd):
    return jnp.where(odd, x, right_of(x, steps))


def go_down(fine, coarse, depth, shape):
    steps = 1 << depth
    count = shape.slabs(depth + 1)
    odd = (lane_index(shape.lanes) & steps) != 0
    a_f, b_f, gd_f, gr_f, v_f = (fine[k] for k in ("a", "b", "gd", "gr", "est"))
    last_level = depth + 1 == GRIDS

    def down_part(k):
        a = a_f[2 * k + 1]
        flux = gd_f[2 * k + 1] + a * (v_f[2 * k + 2] - v_f[2 * k + 1])
        return pair_sum(a, steps, odd), pair_sum(flux, steps, odd)

    def step(k, carry):
        a_prev, gd_prev = carry
        a, gd = down_part(k)
        v0, v1 = v_f[2 * k], v_f[2 * k + 1]
        b0, b1 = b_f[2 * k], b_f[2 * k + 1]
        fr = gr_f[2 * k] + gr_f[2 * k + 1] + b0 * (right_of(v0, steps) - v0) + b1 * (right_of(v1, steps) - v1)
        b = odd_value(b0 + b1, steps, odd)
        gr = odd_value(fr, steps, odd)
        right_side = gd - gd_prev + gr - left_of(gr, 2 * steps)
        if last_level:
            coarse["w"][k] = a + b
            coarse["est"][k] = right_side
        else:
            w = relax_weight(a + a_prev + b + left_of(b, 2 * steps))
            put_level(coarse, k, a, b, gd, gr, w, w * right_side)
        return a, gd

    a, gd = down_part(count - 1)
    run(count, step, (chunk_above(a), chunk_above(gd)))
    if not last_level:
        close(coarse["est"], count)


def lane_select(shape):
    place = lax.broadcasted_iota(jnp.int32, (shape.cols, LANE), 0)
    target = lax.broadcasted_iota(jnp.int32, (shape.cols, LANE), 1)
    return (place == target * CELL).astype(jnp.bfloat16)


def three_parts(x):
    high = x.astype(jnp.bfloat16)
    rest = x - high.astype(jnp.float32)
    middle = rest.astype(jnp.bfloat16)
    low = (rest - middle.astype(jnp.float32)).astype(jnp.bfloat16)
    return high, middle, low


def select_product(x, one_hot):
    n = x.shape[0]
    parts = jnp.concatenate(list(three_parts(x)), axis=0)
    out = jnp.dot(parts, one_hot, preferred_element_type=jnp.float32)
    return out[0:n] + out[n : 2 * n] + out[2 * n : 3 * n]


def publish(coarse, out, shape):
    per = shape.per_chunk
    weights = sum(coarse["w"][j][:, : shape.cols] for j in range(per))
    fields = [coarse["est"][j][:, : shape.cols] for j in range(per)] + [weights]
    packed = select_product(jnp.concatenate(fields, axis=0), lane_select(shape))
    block = packed[0:SUB]
    for j in range(1, per + 1):
        block = block + pltpu.roll(packed[j * SUB : (j + 1) * SUB], j * shape.ccols, 1)
    for device in range(shape.row_count * shape.col_count):
        out[device] = block


LEVEL_KEYS = ("a", "b", "gd", "gr", "w", "est")


def levels_down(level0, levels, last, out, shape):
    chain = [level0] + levels + [last]
    for depth in range(GRIDS):
        go_down(chain[depth], chain[depth + 1], depth, shape)
    publish(last, out, shape)


def coarse_correction(gathered, tables, shape, corr):
    table, forward_x, backward_x, inverse = tables
    rows, cols = shape.row_count, shape.col_count
    per, crows, ccols = shape.per_chunk, shape.crows, shape.ccols
    gr, gc = shape.grid_rows, shape.grid_cols
    group = LANE // ccols
    lane = lane_index(LANE)
    blocks = []
    for j in range(per):
        for r in range(rows):
            pieces = []
            for tile in range(cols // group):
                piece = None
                for g in range(group):
                    x = gathered[r * cols + tile * group + g]
                    shift = ((g - j) * ccols) % LANE
                    x = pltpu.roll(x, shift, 1) if shift else x
                    piece = x if piece is None else jnp.where(lane >= g * ccols, x, piece)
                pieces.append(piece)
            blocks.append(jnp.concatenate(pieces, axis=1))
    strip = jnp.concatenate(blocks, axis=0)

    weights = gathered[0]
    for device in range(1, rows * cols):
        weights = weights + gathered[device]
    sub = lax.broadcasted_iota(jnp.int32, (SUB, LANE), 0)
    own = (sub < crows // per) & (lane >= per * ccols) & (lane < (per + 1) * ccols)
    total = jnp.sum(jnp.where(own, weights, 0.0), keepdims=True)
    count = (gr - 1) * gc + gr * (gc - 1)
    mean = total / count + epsilon

    spectrum = lax.dot_general(strip, table[...], (((1,), (1,)), ((), ())), precision=highest)
    spectrum = jnp.dot(forward_x[...], spectrum, precision=highest)
    spectrum = spectrum * (inverse[...] / mean)
    values = jnp.dot(backward_x[lax.axis_index("row")], spectrum, precision=highest)
    values = jnp.dot(values, table[...], precision=highest)

    def at(dim, size):
        return lax.broadcasted_iota(jnp.int32, size, dim)

    size = (gc, shape.lanes)
    cell = at(1, size) // CELL
    edge = (shape.cols + COL_HALO) // CELL
    cell = jnp.where(cell < edge, cell, cell - shape.lanes // CELL)
    spread = (at(0, size) == cell + lax.axis_index("col") * ccols).astype(jnp.bfloat16)
    values = select_product(values, spread)
    for j in range(per):
        corr[j] = values[j * SUB : (j + 1) * SUB]
    close(corr, per)


def go_up(level, corr, depth, shape, emit):
    steps = 1 << depth
    count = shape.slabs(depth)
    a_r, b_r, gd_r, gr_r, w_r, e_r = (level[k] for k in LEVEL_KEYS)

    def down_flux(i, v, v_next):
        return gd_r[i] + a_r[i] * (v_next - v)

    def sweep(i, v, v_next, f_prev):
        fd = down_flux(i, v, v_next)
        fr = gr_r[i] + b_r[i] * (right_of(v, steps) - v)
        emit(i, v + w_r[i] * (fd - f_prev + fr - left_of(fr, steps)))
        return fd

    def pair(k, carry):
        v0, f_prev = carry
        v1 = e_r[2 * k + 1] + corr[k]
        v2 = e_r[2 * k + 2] + corr[k + 1]
        f_prev = sweep(2 * k, v0, v1, f_prev)
        return v2, sweep(2 * k + 1, v1, v2, f_prev)

    v_last = e_r[count - 1] + corr[count // 2 - 1]
    v_wrap = e_r[count] + corr[count // 2]
    f_prev = chunk_above(down_flux(count - 1, v_last, v_wrap))
    run(count // 2, pair, (e_r[0] + corr[0], f_prev))


def levels_up(levels, corr, results, shape):
    for depth in range(GRIDS - 1, 0, -1):
        out = results[depth - 1]

        def emit(i, value, out=out):
            out[i] = value

        go_up(levels[depth - 1], corr, depth, shape, emit)
        close(out, shape.slabs(depth))
        corr = out
    return corr


def as_levels(refs):
    n = len(LEVEL_KEYS)
    return [dict(zip(LEVEL_KEYS, refs[i : i + n])) for i in range(0, len(refs), n)]


def start_kernel(*refs, shape):
    (quality, counts, above, below, from_right, from_left) = refs[:6]
    out = refs[6]
    sd_r, sr_r = refs[7:9]
    level_refs = refs[9 : 9 + 6 * GRIDS]
    nat_q, nat_n, q_r, n_r, rhs, wsum = refs[9 + 6 * GRIDS :]
    rows, ext, tiles = shape.rows, shape.ext_rows, shape.tiles
    level0, *levels = as_levels(level_refs)

    for t in range(tiles):
        lanes = slice(t * LANE, (t + 1) * LANE)
        nat_q[t, 0:rows, :] = quality[:, lanes]
        nat_n[t, 0:rows, :] = counts[:, lanes]
        for ref, start in ((below, rows), (above, ext - ROW_HALO)):
            nat_q[t, start : start + ROW_HALO, :] = ref[0:ROW_HALO, lanes]
            nat_n[t, start : start + ROW_HALO, :] = ref[ROW_HALO : 2 * ROW_HALO, lanes]
        if ext > rows + 2 * ROW_HALO:
            gap = slice(rows + ROW_HALO, ext - ROW_HALO)
            nat_q[t, gap, :] = jnp.zeros_like(nat_q[t, gap, :])
            nat_n[t, gap, :] = jnp.zeros_like(nat_n[t, gap, :])
    low = lane_index(LANE) < COL_HALO
    count = shape.chunk

    def relay(i, carry):
        rows_of = pl.ds(i, SUB, stride=shape.chunk)
        right, left = from_right[rows_of, :], from_left[rows_of, :]
        q = [nat_q[t, rows_of, :] for t in range(tiles)] + [jnp.where(low, right, left)]
        n = [nat_n[t, rows_of, :] for t in range(tiles)]
        n += [pltpu.roll(jnp.where(low, left, right), COL_HALO, 1)]
        q_r[i] = jnp.concatenate(q, axis=1)
        n_r[i] = jnp.concatenate(n, axis=1)
        return carry

    run(count, relay, 0)
    close(q_r, count)
    close(n_r, count)

    def down_part(i):
        a = jnp.minimum(q_r[i], q_r[i + 1])
        sd = wrap_steps(n_r[i + 1] - n_r[i])
        return a, sd, -(a * sd)

    def step(i, carry):
        a_prev, gd_prev = carry
        a, sd, gd = down_part(i)
        q, n = q_r[i], n_r[i]
        b = jnp.minimum(q, right_of(q, 1))
        sr = wrap_steps(right_of(n, 1) - n)
        gr = -(b * sr)
        w = relax_weight(a + a_prev + b + left_of(b, 1))
        put_level(level0, i, a, b, gd, gr, w, w * (gd - gd_prev + gr - left_of(gr, 1)))
        sd_r[i] = sd
        sr_r[i] = sr
        return a, gd

    a, _, gd = down_part(count - 1)
    run(count, step, (chunk_above(a), chunk_above(gd)))
    close(level0["est"], count)
    levels_down(level0, levels, dict(est=rhs, w=wsum), out, shape)


def middle_kernel(*refs, shape):
    gathered, tables, (sd_r, sr_r) = refs[0], refs[1:5], refs[5:7]
    old = as_levels(refs[7 : 7 + 6 * GRIDS])
    refs = refs[7 + 6 * GRIDS :]
    out, first = refs[:2]
    level0, *levels = as_levels(refs[2 : 2 + 6 * GRIDS])
    rhs, wsum, corr, *results = refs[2 + 6 * GRIDS :]
    coarse_correction(gathered, tables, shape, corr)
    field = levels_up(old[1:], corr, results, shape)

    def emit(i, value):
        first[i] = value

    count = shape.chunk
    go_up(old[0], field, 0, shape, emit)
    close(first, count)
    a_old, b_old = old[0]["a"], old[0]["b"]

    def down_part(i):
        error = first[i + 1] - first[i] - sd_r[i]
        a = a_old[i] / jnp.maximum(jnp.abs(error), error_floor)
        return a, a * error

    def step(i, carry):
        a_prev, gd_prev = carry
        a, gd = down_part(i)
        v = first[i]
        error = right_of(v, 1) - v - sr_r[i]
        b = b_old[i] / jnp.maximum(jnp.abs(error), error_floor)
        gr = b * error
        w = relax_weight(a + a_prev + b + left_of(b, 1))
        put_level(level0, i, a, b, gd, gr, w, w * (gd - gd_prev + gr - left_of(gr, 1)))
        return a, gd

    a, gd = down_part(count - 1)
    run(count, step, (chunk_above(a), chunk_above(gd)))
    close(level0["est"], count)
    levels_down(level0, levels, dict(est=rhs, w=wsum), out, shape)


def end_kernel(*refs, shape):
    gathered, tables, first = refs[0], refs[1:5], refs[5]
    old = as_levels(refs[6 : 6 + 6 * GRIDS])
    out, nat, corr, *results = refs[6 + 6 * GRIDS :]
    coarse_correction(gathered, tables, shape, corr)
    field = levels_up(old[1:], corr, results, shape)

    def emit(i, value):
        value = value + first[i]
        for t in range(shape.tiles):
            nat[t, pl.ds(i, SUB, stride=shape.chunk), :] = value[:, t * LANE : (t + 1) * LANE]

    go_up(old[0], field, 0, shape, emit)
    for t in range(shape.tiles):
        out[:, t * LANE : (t + 1) * LANE] = nat[t, 0 : shape.rows, :]


def dct_table(count):
    freq = np.arange(count)[:, None]
    place = np.arange(count)[None, :]
    table = np.cos(np.pi * (((2 * place + 1) * freq) % (4 * count)) / (2 * count)) * np.sqrt(2.0 / count)
    table[0] *= np.sqrt(0.5)
    return table.astype(np.float32)


def solve_tables(shape):
    gr, gc, per, crows = shape.grid_rows, shape.grid_cols, shape.per_chunk, shape.crows
    table_x = dct_table(gr)
    slab, row, chunk = np.meshgrid(np.arange(per), np.arange(shape.row_count), np.arange(SUB), indexing="ij")
    inside = (chunk < crows // per).ravel()
    place = (row * crows + chunk * per + slab).ravel()
    forward = np.where(inside, table_x[:, np.where(inside, place, 0)], 0)
    slab, chunk = np.meshgrid(np.arange(per), np.arange(SUB), indexing="ij")
    local = (chunk * per + slab).ravel()
    slots = SUB * per
    local = np.where(local < slots - ROW_HALO // CELL, local, local - slots)
    backward = [table_x.T[np.clip(r * crows + local, 0, gr - 1)] for r in range(shape.row_count)]
    lam_x = 2 - 2 * np.cos(np.pi * np.arange(gr) / gr)
    lam_y = 2 - 2 * np.cos(np.pi * np.arange(gc) / gc)
    inverse = 1 / (lam_x[:, None] + lam_y[None, :] + (screen_width / gc) ** 2)
    return [jnp.asarray(x, jnp.float32) for x in (dct_table(gc), forward, np.stack(backward), inverse)]


def f32(*dims):
    return jax.ShapeDtypeStruct(dims, jnp.float32)


def level_shapes(shape):
    return [
        f32(shape.slabs(d) + (key == "est"), SUB, shape.lanes) for d in range(GRIDS) for key in LEVEL_KEYS
    ]


def vmem(*dims):
    return pltpu.VMEM(dims, jnp.float32)


def exchange(lower, upper, axis):
    count = lax.axis_size(axis)
    up = [(i, i + 1) for i in range(count - 1)]
    down = [(i + 1, i) for i in range(count - 1)]
    return lax.ppermute(upper, axis, up), lax.ppermute(lower, axis, down)


def body(swath, coherence, phase_counts, *, shape):
    params = pltpu.CompilerParams(vmem_limit_bytes=16 * 2**20)
    rows, cols = shape.rows, shape.cols
    block = f32(shape.row_count * shape.col_count, SUB, LANE)
    tables = solve_tables(shape)
    coarse_scratch = [vmem(shape.per_chunk, SUB, shape.lanes)] * 2
    result_scratch = [vmem(shape.per_chunk + 1, SUB, shape.lanes)]
    result_scratch += [vmem(shape.slabs(d) + 1, SUB, shape.lanes) for d in range(1, GRIDS)]

    strip = f32(2 * ROW_HALO, cols)
    quality, counts, top, bottom = pl.pallas_call(
        strips_kernel,
        in_specs=[pl.BlockSpec(memory_space=pltpu.HBM)] * 3,
        out_shape=[f32(rows, cols), f32(rows, cols), strip, strip],
        scratch_shapes=[pltpu.VMEM((rows, cols), jnp.int32)] * 3 + [pltpu.SemaphoreType.DMA((3,))],
        compiler_params=params,
        name="row_strips",
    )(swath, coherence, phase_counts)
    above, below = exchange(top, bottom, "row")
    strip = f32(shape.ext_rows, LANE)
    first_cols, last_cols = pl.pallas_call(
        functools.partial(col_strip_kernel, shape=shape),
        out_shape=[strip, strip],
        compiler_params=params,
        name="col_strips",
    )(quality, counts, above, below)
    from_left, from_right = exchange(first_cols, last_cols, "col")

    slabs = (shape.chunk, SUB, shape.lanes)
    more = (shape.chunk + 1, SUB, shape.lanes)
    nat = vmem(shape.tiles, shape.ext_rows, LANE)
    block_out, sd, sr, *old = pl.pallas_call(
        functools.partial(start_kernel, shape=shape),
        out_shape=[block, f32(*slabs), f32(*slabs)] + level_shapes(shape),
        scratch_shapes=[nat, nat, vmem(*more), vmem(*more)] + coarse_scratch,
        compiler_params=params,
        name="start",
    )(quality, counts, above, below, from_right, from_left)
    gathered = lax.all_to_all(block_out, ("row", "col"), split_axis=0, concat_axis=0, tiled=True)
    block_out, first, *old = pl.pallas_call(
        functools.partial(middle_kernel, shape=shape),
        out_shape=[block, f32(*more)] + level_shapes(shape),
        scratch_shapes=coarse_scratch + result_scratch,
        compiler_params=params,
        name="middle",
    )(gathered, *tables, sd, sr, *old)
    gathered = lax.all_to_all(block_out, ("row", "col"), split_axis=0, concat_axis=0, tiled=True)
    return pl.pallas_call(
        functools.partial(end_kernel, shape=shape),
        out_shape=f32(rows, cols),
        scratch_shapes=[nat] + result_scratch,
        compiler_params=params,
        name="finish",
    )(gathered, *tables, first, *old)


def solution(mesh):
    def run(swath, coherence, phase_counts):
        rows, cols = swath.shape
        row_count, col_count = mesh.shape["row"], mesh.shape["col"]
        shape = Shape(rows // row_count, cols // col_count, row_count, col_count)
        return jax.shard_map(
            functools.partial(body, shape=shape),
            mesh=mesh,
            in_specs=(P("row", "col"), P("row", "col"), P("row", "col")),
            out_specs=P("row", "col"),
            check_vma=False,
        )(swath, coherence, phase_counts)

    return run
```

```python
import functools

import jax
import jax.numpy as jnp
import numpy as np
from jax import lax
from jax.experimental import pallas as pl
from jax.experimental.pallas import tpu as pltpu
from jax.sharding import PartitionSpec as P

GRIDS = 4
LEVELS = 256
NCLASS = 8

damping = 0.8
diag_floor = 0.5
error_floor = 0.5
epsilon = 1e-06
screen_width = 4.0
highest = lax.Precision.HIGHEST

UNROLL = 4
WHOLE = 8

CELL = 2**GRIDS
ROW_HALO = 3 * CELL
COL_HALO = 64
SUB = 8
LANE = 128


class Shape:
    def __init__(self, rows, cols, row_count, col_count):
        self.rows, self.cols = rows, cols
        self.row_count, self.col_count = row_count, col_count
        unit = SUB * CELL
        self.ext_rows = -(-(rows + 2 * ROW_HALO) // unit) * unit
        self.lanes = cols + 2 * COL_HALO
        self.chunk = self.ext_rows // SUB
        self.tiles = cols // LANE
        self.crows, self.ccols = rows // CELL, cols // CELL
        self.per_chunk = self.chunk // CELL
        self.grid_rows = self.crows * row_count
        self.grid_cols = self.ccols * col_count

    def slabs(self, depth):
        return self.chunk >> depth


def quality_of(swath, coherence):
    scaled = coherence.astype(jnp.float32) / (NCLASS - 1)
    return swath.astype(jnp.float32) * (scaled * scaled)


def lane_index(width):
    return lax.broadcasted_iota(jnp.int32, (SUB, width), 1)


def right_of(x, steps):
    return pltpu.roll(x, x.shape[1] - steps, 1)


def left_of(x, steps):
    return pltpu.roll(x, steps, 1)


def chunk_below(x):
    return pltpu.roll(x, SUB - 1, 0)


def chunk_above(x):
    return pltpu.roll(x, 1, 0)


def wrap_steps(difference):
    turns = jnp.floor(difference * (1.0 / LEVELS) + 0.5)
    return (difference - LEVELS * turns) * (2.0 * jnp.pi / LEVELS)


def relax_weight(diagonal):
    return damping / jnp.maximum(diagonal, diag_floor)


def position(axis):
    index, count = lax.axis_index(axis), lax.axis_size(axis)
    return index % 2 == 0, (index == 0) | (index == count - 1)


def aligned(start):
    return pl.multiple_of(start, SUB)


def strips_kernel(
    swath, coherence, counts, quality, phase, row_even, row_odd, col_even, col_odd, s_buf, c_buf, p_buf, sems
):
    rows, cols = quality.shape
    copies = [
        pltpu.make_async_copy(src, dst, sems.at[n])
        for n, (src, dst) in enumerate(((swath, s_buf), (coherence, c_buf), (counts, p_buf)))
    ]
    for copy in copies:
        copy.start()
    for copy in copies:
        copy.wait()
    for r in range(0, rows, 2 * SUB):
        here = slice(r, r + 2 * SUB)
        quality[here, :] = quality_of(s_buf[here, :], c_buf[here, :])
        phase[here, :] = p_buf[here, :].astype(jnp.float32)
    even, _ = position("row")
    bottom = rows - ROW_HALO
    for out, start in ((row_even, jnp.where(even, bottom, 0)), (row_odd, jnp.where(even, 0, bottom))):
        here = pl.ds(aligned(start), ROW_HALO)
        out[0:ROW_HALO, :] = quality[here, :]
        out[ROW_HALO : 2 * ROW_HALO, :] = phase[here, :]
    even, _ = position("col")
    low = lax.broadcasted_iota(jnp.int32, (1, LANE), 1) < COL_HALO
    left, right = slice(0, LANE), slice(cols - LANE, cols)
    first = jnp.where(low, quality[:, left], pltpu.roll(phase[:, left], COL_HALO, 1))
    last = jnp.where(low, pltpu.roll(phase[:, right], COL_HALO, 1), quality[:, right])
    col_even[...] = jnp.where(even, last, first)
    col_odd[...] = jnp.where(even, first, last)


def corner_kernel(col_even, col_odd, quality, phase, row_even, row_odd):
    rows = quality.shape[0]
    even, at_end = position("col")
    low = lax.broadcasted_iota(jnp.int32, (1, LANE), 1) < COL_HALO
    met = col_even[...]
    other = jnp.where(at_end, 0.0, col_odd[...])
    right = jnp.where(even, met, other)
    left = jnp.where(even, other, met)
    quality[...] = jnp.where(low, right, left)
    phase[...] = pltpu.roll(jnp.where(low, left, right), COL_HALO, 1)
    even, _ = position("row")
    bottom = rows - ROW_HALO
    for out, start in ((row_even, jnp.where(even, bottom, 0)), (row_odd, jnp.where(even, 0, bottom))):
        here = pl.ds(aligned(start), ROW_HALO)
        out[0:ROW_HALO, :] = quality[here, :]
        out[ROW_HALO : 2 * ROW_HALO, :] = phase[here, :]


def run(count, step, carry):
    unroll = min(count, UNROLL)
    if count <= WHOLE:
        for i in range(count):
            carry = step(i, carry)
        return carry

    def turn(t, carry):
        for u in range(unroll):
            carry = step(t * unroll + u, carry)
        return carry

    carry = lax.fori_loop(0, count // unroll, turn, carry)
    for i in range(count // unroll * unroll, count):
        carry = step(i, carry)
    return carry


def close(field, count):
    field[count] = chunk_below(field[0])


def put_level(level, i, *values):
    for key, value in zip(LEVEL_KEYS, values):
        level[key][i] = value


def pair_sum(x, steps, odd):
    y = x + right_of(x, steps)
    return jnp.where(odd, left_of(y, steps), y)


def odd_value(x, steps, odd):
    return jnp.where(odd, x, right_of(x, steps))


def go_down(fine, coarse, depth, shape):
    steps = 1 << depth
    count = shape.slabs(depth + 1)
    odd = (lane_index(shape.lanes) & steps) != 0
    a_f, b_f, gd_f, gr_f, v_f = (fine[k] for k in ("a", "b", "gd", "gr", "est"))
    last_level = depth + 1 == GRIDS

    def down_part(k):
        a = a_f[2 * k + 1]
        flux = gd_f[2 * k + 1] + a * (v_f[2 * k + 2] - v_f[2 * k + 1])
        return pair_sum(a, steps, odd), pair_sum(flux, steps, odd)

    def step(k, carry):
        a_prev, gd_prev = carry
        a, gd = down_part(k)
        v0, v1 = v_f[2 * k], v_f[2 * k + 1]
        b0, b1 = b_f[2 * k], b_f[2 * k + 1]
        fr = gr_f[2 * k] + gr_f[2 * k + 1] + b0 * (right_of(v0, steps) - v0) + b1 * (right_of(v1, steps) - v1)
        b = odd_value(b0 + b1, steps, odd)
        gr = odd_value(fr, steps, odd)
        right_side = gd - gd_prev + gr - left_of(gr, 2 * steps)
        if last_level:
            coarse["w"][k] = a + b
            coarse["est"][k] = right_side
        else:
            w = relax_weight(a + a_prev + b + left_of(b, 2 * steps))
            put_level(coarse, k, a, b, gd, gr, w, w * right_side)
        return a, gd

    a, gd = down_part(count - 1)
    run(count, step, (chunk_above(a), chunk_above(gd)))
    if not last_level:
        close(coarse["est"], count)


def lane_select(shape):
    place = lax.broadcasted_iota(jnp.int32, (shape.cols, LANE), 0)
    target = lax.broadcasted_iota(jnp.int32, (shape.cols, LANE), 1)
    return (place == target * CELL).astype(jnp.bfloat16)


def three_parts(x):
    high = x.astype(jnp.bfloat16)
    rest = x - high.astype(jnp.float32)
    middle = rest.astype(jnp.bfloat16)
    low = (rest - middle.astype(jnp.float32)).astype(jnp.bfloat16)
    return high, middle, low


def select_product(x, one_hot):
    n = x.shape[0]
    parts = jnp.concatenate(list(three_parts(x)), axis=0)
    out = jnp.dot(parts, one_hot, preferred_element_type=jnp.float32)
    return out[0:n] + out[n : 2 * n] + out[2 * n : 3 * n]


def publish(coarse, out, shape):
    per = shape.per_chunk
    weights = sum(coarse["w"][j][:, : shape.cols] for j in range(per))
    fields = [coarse["est"][j][:, : shape.cols] for j in range(per)] + [weights]
    packed = select_product(jnp.concatenate(fields, axis=0), lane_select(shape))
    block = packed[0:SUB]
    for j in range(1, per + 1):
        block = block + pltpu.roll(packed[j * SUB : (j + 1) * SUB], j * shape.ccols, 1)
    for device in range(shape.row_count * shape.col_count):
        out[device] = block


LEVEL_KEYS = ("a", "b", "gd", "gr", "w", "est")


def levels_down(level0, levels, last, out, shape):
    chain = [level0] + levels + [last]
    for depth in range(GRIDS):
        go_down(chain[depth], chain[depth + 1], depth, shape)
    publish(last, out, shape)


def coarse_correction(gathered, tables, shape, corr):
    table, forward_x, backward_x, inverse = tables
    rows, cols = shape.row_count, shape.col_count
    per, crows, ccols = shape.per_chunk, shape.crows, shape.ccols
    gr, gc = shape.grid_rows, shape.grid_cols
    group = LANE // ccols
    lane = lane_index(LANE)
    blocks = []
    for j in range(per):
        for r in range(rows):
            pieces = []
            for tile in range(cols // group):
                piece = None
                for g in range(group):
                    x = gathered[r * cols + tile * group + g]
                    shift = ((g - j) * ccols) % LANE
                    x = pltpu.roll(x, shift, 1) if shift else x
                    piece = x if piece is None else jnp.where(lane >= g * ccols, x, piece)
                pieces.append(piece)
            blocks.append(jnp.concatenate(pieces, axis=1))
    strip = jnp.concatenate(blocks, axis=0)

    weights = gathered[0]
    for device in range(1, rows * cols):
        weights = weights + gathered[device]
    sub = lax.broadcasted_iota(jnp.int32, (SUB, LANE), 0)
    own = (sub < crows // per) & (lane >= per * ccols) & (lane < (per + 1) * ccols)
    total = jnp.sum(jnp.where(own, weights, 0.0), keepdims=True)
    count = (gr - 1) * gc + gr * (gc - 1)
    mean = total / count + epsilon

    spectrum = lax.dot_general(strip, table[...], (((1,), (1,)), ((), ())), precision=highest)
    spectrum = jnp.dot(forward_x[...], spectrum, precision=highest)
    spectrum = spectrum * (inverse[...] / mean)
    values = jnp.dot(backward_x[lax.axis_index("row")], spectrum, precision=highest)
    values = jnp.dot(values, table[...], precision=highest)

    def at(dim, size):
        return lax.broadcasted_iota(jnp.int32, size, dim)

    size = (gc, shape.lanes)
    cell = at(1, size) // CELL
    edge = (shape.cols + COL_HALO) // CELL
    cell = jnp.where(cell < edge, cell, cell - shape.lanes // CELL)
    spread = (at(0, size) == cell + lax.axis_index("col") * ccols).astype(jnp.bfloat16)
    values = select_product(values, spread)
    for j in range(per):
        corr[j] = values[j * SUB : (j + 1) * SUB]
    close(corr, per)


def go_up(level, corr, depth, shape, emit):
    steps = 1 << depth
    count = shape.slabs(depth)
    a_r, b_r, gd_r, gr_r, w_r, e_r = (level[k] for k in LEVEL_KEYS)

    def down_flux(i, v, v_next):
        return gd_r[i] + a_r[i] * (v_next - v)

    def sweep(i, v, v_next, f_prev):
        fd = down_flux(i, v, v_next)
        fr = gr_r[i] + b_r[i] * (right_of(v, steps) - v)
        emit(i, v + w_r[i] * (fd - f_prev + fr - left_of(fr, steps)))
        return fd

    def pair(k, carry):
        v0, f_prev = carry
        v1 = e_r[2 * k + 1] + corr[k]
        v2 = e_r[2 * k + 2] + corr[k + 1]
        f_prev = sweep(2 * k, v0, v1, f_prev)
        return v2, sweep(2 * k + 1, v1, v2, f_prev)

    v_last = e_r[count - 1] + corr[count // 2 - 1]
    v_wrap = e_r[count] + corr[count // 2]
    f_prev = chunk_above(down_flux(count - 1, v_last, v_wrap))
    run(count // 2, pair, (e_r[0] + corr[0], f_prev))


def levels_up(levels, corr, results, shape):
    for depth in range(GRIDS - 1, 0, -1):
        out = results[depth - 1]

        def emit(i, value, out=out):
            out[i] = value

        go_up(levels[depth - 1], corr, depth, shape, emit)
        close(out, shape.slabs(depth))
        corr = out
    return corr


def as_levels(refs):
    n = len(LEVEL_KEYS)
    return [dict(zip(LEVEL_KEYS, refs[i : i + n])) for i in range(0, len(refs), n)]


def start_kernel(*refs, shape):
    (quality, counts, row_even, row_odd, edge_q, edge_n, corner_even, corner_odd) = refs[:8]
    out = refs[8]
    sd_r, sr_r = refs[9:11]
    level_refs = refs[11 : 11 + 6 * GRIDS]
    nat_q, nat_n, q_r, n_r, rhs, wsum = refs[11 + 6 * GRIDS :]
    rows, ext, tiles = shape.rows, shape.ext_rows, shape.tiles
    level0, *levels = as_levels(level_refs)

    even, at_end = position("row")
    below, above = rows, ext - ROW_HALO
    met = pl.ds(aligned(jnp.where(even, below, above)), ROW_HALO)
    other = pl.ds(aligned(jnp.where(even, above, below)), ROW_HALO)
    for t in range(tiles + 1):
        lanes = slice(t * LANE, (t + 1) * LANE) if t < tiles else slice(0, LANE)
        own_q, own_n, from_even, from_odd = (
            (quality, counts, row_even, row_odd) if t < tiles else (edge_q, edge_n, corner_even, corner_odd)
        )
        for nat, own, start in ((nat_q, own_q, 0), (nat_n, own_n, ROW_HALO)):
            nat[t, 0:rows, :] = own[:, lanes]
            nat[t, met, :] = from_even[start : start + ROW_HALO, lanes]
            nat[t, other, :] = jnp.where(at_end, 0.0, from_odd[start : start + ROW_HALO, lanes])
            if ext > rows + 2 * ROW_HALO:
                gap = slice(rows + ROW_HALO, ext - ROW_HALO)
                nat[t, gap, :] = jnp.zeros_like(nat[t, gap, :])
    count = shape.chunk

    def relay(i, carry):
        rows_of = pl.ds(i, SUB, stride=shape.chunk)
        q_r[i] = jnp.concatenate([nat_q[t, rows_of, :] for t in range(tiles + 1)], axis=1)
        n_r[i] = jnp.concatenate([nat_n[t, rows_of, :] for t in range(tiles + 1)], axis=1)
        return carry

    run(count, relay, 0)
    close(q_r, count)
    close(n_r, count)

    def down_part(i):
        a = jnp.minimum(q_r[i], q_r[i + 1])
        sd = wrap_steps(n_r[i + 1] - n_r[i])
        return a, sd, -(a * sd)

    def step(i, carry):
        a_prev, gd_prev = carry
        a, sd, gd = down_part(i)
        q, n = q_r[i], n_r[i]
        b = jnp.minimum(q, right_of(q, 1))
        sr = wrap_steps(right_of(n, 1) - n)
        gr = -(b * sr)
        w = relax_weight(a + a_prev + b + left_of(b, 1))
        put_level(level0, i, a, b, gd, gr, w, w * (gd - gd_prev + gr - left_of(gr, 1)))
        sd_r[i] = sd
        sr_r[i] = sr
        return a, gd

    a, _, gd = down_part(count - 1)
    run(count, step, (chunk_above(a), chunk_above(gd)))
    close(level0["est"], count)
    levels_down(level0, levels, dict(est=rhs, w=wsum), out, shape)


def middle_kernel(*refs, shape):
    gathered, tables, (sd_r, sr_r) = refs[0], refs[1:5], refs[5:7]
    old = as_levels(refs[7 : 7 + 6 * GRIDS])
    refs = refs[7 + 6 * GRIDS :]
    out, first = refs[:2]
    level0, *levels = as_levels(refs[2 : 2 + 6 * GRIDS])
    rhs, wsum, corr, *results = refs[2 + 6 * GRIDS :]
    coarse_correction(gathered, tables, shape, corr)
    field = levels_up(old[1:], corr, results, shape)

    def emit(i, value):
        first[i] = value

    count = shape.chunk
    go_up(old[0], field, 0, shape, emit)
    close(first, count)
    a_old, b_old = old[0]["a"], old[0]["b"]

    def down_part(i):
        error = first[i + 1] - first[i] - sd_r[i]
        a = a_old[i] / jnp.maximum(jnp.abs(error), error_floor)
        return a, a * error

    def step(i, carry):
        a_prev, gd_prev = carry
        a, gd = down_part(i)
        v = first[i]
        error = right_of(v, 1) - v - sr_r[i]
        b = b_old[i] / jnp.maximum(jnp.abs(error), error_floor)
        gr = b * error
        w = relax_weight(a + a_prev + b + left_of(b, 1))
        put_level(level0, i, a, b, gd, gr, w, w * (gd - gd_prev + gr - left_of(gr, 1)))
        return a, gd

    a, gd = down_part(count - 1)
    run(count, step, (chunk_above(a), chunk_above(gd)))
    close(level0["est"], count)
    levels_down(level0, levels, dict(est=rhs, w=wsum), out, shape)


def end_kernel(*refs, shape):
    gathered, tables, first = refs[0], refs[1:5], refs[5]
    old = as_levels(refs[6 : 6 + 6 * GRIDS])
    out, nat, corr, *results = refs[6 + 6 * GRIDS :]
    coarse_correction(gathered, tables, shape, corr)
    field = levels_up(old[1:], corr, results, shape)

    def emit(i, value):
        value = value + first[i]
        for t in range(shape.tiles):
            nat[t, pl.ds(i, SUB, stride=shape.chunk), :] = value[:, t * LANE : (t + 1) * LANE]

    go_up(old[0], field, 0, shape, emit)
    for t in range(shape.tiles):
        out[:, t * LANE : (t + 1) * LANE] = nat[t, 0 : shape.rows, :]


def dct_table(count):
    freq = np.arange(count)[:, None]
    place = np.arange(count)[None, :]
    table = np.cos(np.pi * (((2 * place + 1) * freq) % (4 * count)) / (2 * count)) * np.sqrt(2.0 / count)
    table[0] *= np.sqrt(0.5)
    return table.astype(np.float32)


def solve_tables(shape):
    gr, gc, per, crows = shape.grid_rows, shape.grid_cols, shape.per_chunk, shape.crows
    table_x = dct_table(gr)
    slab, row, chunk = np.meshgrid(np.arange(per), np.arange(shape.row_count), np.arange(SUB), indexing="ij")
    inside = (chunk < crows // per).ravel()
    place = (row * crows + chunk * per + slab).ravel()
    forward = np.where(inside, table_x[:, np.where(inside, place, 0)], 0)
    slab, chunk = np.meshgrid(np.arange(per), np.arange(SUB), indexing="ij")
    local = (chunk * per + slab).ravel()
    slots = SUB * per
    local = np.where(local < slots - ROW_HALO // CELL, local, local - slots)
    backward = [table_x.T[np.clip(r * crows + local, 0, gr - 1)] for r in range(shape.row_count)]
    lam_x = 2 - 2 * np.cos(np.pi * np.arange(gr) / gr)
    lam_y = 2 - 2 * np.cos(np.pi * np.arange(gc) / gc)
    inverse = 1 / (lam_x[:, None] + lam_y[None, :] + (screen_width / gc) ** 2)
    return [jnp.asarray(x, jnp.float32) for x in (dct_table(gc), forward, np.stack(backward), inverse)]


def f32(*dims):
    return jax.ShapeDtypeStruct(dims, jnp.float32)


def level_shapes(shape):
    return [
        f32(shape.slabs(d) + (key == "est"), SUB, shape.lanes) for d in range(GRIDS) for key in LEVEL_KEYS
    ]


def vmem(*dims):
    return pltpu.VMEM(dims, jnp.float32)


def swap(even_strip, odd_strip, axis):
    rows, cols = lax.axis_size("row"), lax.axis_size("col")
    even_pairs, odd_pairs = [], []
    for r in range(rows):
        for c in range(cols):
            here = r * cols + c
            index, count, step = (r, rows, cols) if axis == "row" else (c, cols, 1)
            even_pairs.append((here, here + step * ((index ^ 1) - index)))
            if 0 < index < count - 1:
                odd_pairs.append((here, here + (step if index % 2 else -step)))
            else:
                odd_pairs.append((here, idle_pair(axis, r, c, rows, cols)))
    both = ("row", "col")
    return lax.ppermute(even_strip, both, even_pairs), lax.ppermute(odd_strip, both, odd_pairs)


def idle_pair(axis, r, c, rows, cols):
    if axis == "col":
        return (r ^ 1) * cols + c
    return (rows - 1 - r) * cols + c


def body(swath, coherence, phase_counts, *, shape):
    params = pltpu.CompilerParams(vmem_limit_bytes=16 * 2**20)
    rows, cols = shape.rows, shape.cols
    block = f32(shape.row_count * shape.col_count, SUB, LANE)
    tables = solve_tables(shape)
    coarse_scratch = [vmem(shape.per_chunk, SUB, shape.lanes)] * 2
    result_scratch = [vmem(shape.per_chunk + 1, SUB, shape.lanes)]
    result_scratch += [vmem(shape.slabs(d) + 1, SUB, shape.lanes) for d in range(1, GRIDS)]

    strip, edge, corner = f32(2 * ROW_HALO, cols), f32(rows, LANE), f32(2 * ROW_HALO, LANE)
    quality, counts, row_even, row_odd, col_even, col_odd = pl.pallas_call(
        strips_kernel,
        in_specs=[pl.BlockSpec(memory_space=pltpu.HBM)] * 3,
        out_shape=[f32(rows, cols), f32(rows, cols), strip, strip, edge, edge],
        scratch_shapes=[pltpu.VMEM((rows, cols), jnp.int32)] * 3 + [pltpu.SemaphoreType.DMA((3,))],
        compiler_params=params,
        name="strips",
    )(*(pltpu.with_memory_space_constraint(x, pltpu.HBM) for x in (swath, coherence, phase_counts)))
    row_even, row_odd = swap(row_even, row_odd, "row")
    col_even, col_odd = swap(col_even, col_odd, "col")
    edge_q, edge_n, corner_even, corner_odd = pl.pallas_call(
        corner_kernel,
        out_shape=[edge, edge, corner, corner],
        compiler_params=params,
        name="corners",
    )(col_even, col_odd)
    corner_even, corner_odd = swap(corner_even, corner_odd, "row")

    slabs = (shape.chunk, SUB, shape.lanes)
    more = (shape.chunk + 1, SUB, shape.lanes)
    nat = vmem(shape.tiles, shape.ext_rows, LANE)
    wide = vmem(shape.tiles + 1, shape.ext_rows, LANE)
    block_out, sd, sr, *old = pl.pallas_call(
        functools.partial(start_kernel, shape=shape),
        out_shape=[block, f32(*slabs), f32(*slabs)] + level_shapes(shape),
        scratch_shapes=[wide, wide, vmem(*more), vmem(*more)] + coarse_scratch,
        compiler_params=params,
        name="start",
    )(quality, counts, row_even, row_odd, edge_q, edge_n, corner_even, corner_odd)
    gathered = lax.all_to_all(block_out, ("row", "col"), split_axis=0, concat_axis=0, tiled=True)
    block_out, first, *old = pl.pallas_call(
        functools.partial(middle_kernel, shape=shape),
        out_shape=[block, f32(*more)] + level_shapes(shape),
        scratch_shapes=coarse_scratch + result_scratch,
        compiler_params=params,
        name="middle",
    )(gathered, *tables, sd, sr, *old)
    gathered = lax.all_to_all(block_out, ("row", "col"), split_axis=0, concat_axis=0, tiled=True)
    return pl.pallas_call(
        functools.partial(end_kernel, shape=shape),
        out_shape=f32(rows, cols),
        scratch_shapes=[nat] + result_scratch,
        compiler_params=params,
        name="finish",
    )(gathered, *tables, first, *old)


def solution(mesh):
    def run(swath, coherence, phase_counts):
        rows, cols = swath.shape
        row_count, col_count = mesh.shape["row"], mesh.shape["col"]
        shape = Shape(rows // row_count, cols // col_count, row_count, col_count)
        return jax.shard_map(
            functools.partial(body, shape=shape),
            mesh=mesh,
            in_specs=(P("row", "col"), P("row", "col"), P("row", "col")),
            out_specs=P("row", "col"),
            check_vma=False,
        )(swath, coherence, phase_counts)

    return run
```

```python
import functools

import jax
import jax.numpy as jnp
import numpy as np
from jax import lax
from jax.experimental import pallas as pl
from jax.experimental.pallas import tpu as pltpu
from jax.sharding import PartitionSpec as P

GRIDS = 4
LEVELS = 256
NCLASS = 8

damping = 0.8
diag_floor = 0.5
error_floor = 0.5
epsilon = 1e-06
screen_width = 4.0
highest = lax.Precision.HIGHEST

UNROLL_TOP = 4
UNROLL_DOWN = 4
UNROLL_UP = 4
WHOLE = 8

CELL = 2**GRIDS
ROW_HALO = 3 * CELL
COL_HALO = 64
SUB = 8
LANE = 128


class Shape:
    def __init__(self, rows, cols, row_count, col_count):
        self.rows, self.cols = rows, cols
        self.row_count, self.col_count = row_count, col_count
        unit = SUB * CELL
        self.ext_rows = -(-(rows + 2 * ROW_HALO) // unit) * unit
        self.lanes = cols + 2 * COL_HALO
        self.chunk = self.ext_rows // SUB
        self.tiles = cols // LANE
        self.crows, self.ccols = rows // CELL, cols // CELL
        self.per_chunk = self.chunk // CELL
        self.grid_rows = self.crows * row_count
        self.grid_cols = self.ccols * col_count
        self.group = LANE // self.ccols
        self.block_rows = SUB * self.per_chunk // self.group
        self.fold = SUB // self.block_rows
        assert self.group % self.per_chunk == 0 and self.crows <= self.group * (self.block_rows - 1)
        assert col_count % (self.fold * self.group) == 0 and self.crows % self.per_chunk == 0

    def slabs(self, depth):
        return self.chunk >> depth


def quality_of(swath, coherence):
    scaled = coherence.astype(jnp.float32) / (NCLASS - 1)
    return swath.astype(jnp.float32) * (scaled * scaled)


def lane_index(width):
    return lax.broadcasted_iota(jnp.int32, (SUB, width), 1)


def right_of(x, steps):
    return pltpu.roll(x, x.shape[1] - steps, 1)


def left_of(x, steps):
    return pltpu.roll(x, steps, 1)


def chunk_below(x):
    return pltpu.roll(x, SUB - 1, 0)


def chunk_above(x):
    return pltpu.roll(x, 1, 0)


def wrap_steps(difference):
    turns = jnp.floor(difference * (1.0 / LEVELS) + 0.5)
    return (difference - LEVELS * turns) * (2.0 * jnp.pi / LEVELS)


def relax_weight(diagonal):
    return damping / jnp.maximum(diagonal, diag_floor)


def position(axis):
    index, count = lax.axis_index(axis), lax.axis_size(axis)
    return index % 2 == 0, (index == 0) | (index == count - 1)


def aligned(start):
    return pl.multiple_of(start, SUB)


def strips_kernel(
    swath, coherence, counts, quality, phase, row_even, row_odd, col_even, col_odd, s_buf, c_buf, p_buf, sems
):
    rows, cols = quality.shape
    copies = [
        pltpu.make_async_copy(src, dst, sems.at[n])
        for n, (src, dst) in enumerate(((swath, s_buf), (coherence, c_buf), (counts, p_buf)))
    ]
    for copy in copies:
        copy.start()
    for copy in copies:
        copy.wait()
    for r in range(0, rows, 2 * SUB):
        here = slice(r, r + 2 * SUB)
        quality[here, :] = quality_of(s_buf[here, :], c_buf[here, :])
        phase[here, :] = p_buf[here, :].astype(jnp.float32)
    even, _ = position("row")
    bottom = rows - ROW_HALO
    for out, start in ((row_even, jnp.where(even, bottom, 0)), (row_odd, jnp.where(even, 0, bottom))):
        here = pl.ds(aligned(start), ROW_HALO)
        out[0:ROW_HALO, :] = quality[here, :]
        out[ROW_HALO : 2 * ROW_HALO, :] = phase[here, :]
    even, _ = position("col")
    low = lax.broadcasted_iota(jnp.int32, (1, LANE), 1) < COL_HALO
    left, right = slice(0, LANE), slice(cols - LANE, cols)
    first = jnp.where(low, quality[:, left], pltpu.roll(phase[:, left], COL_HALO, 1))
    last = jnp.where(low, pltpu.roll(phase[:, right], COL_HALO, 1), quality[:, right])
    col_even[...] = jnp.where(even, last, first)
    col_odd[...] = jnp.where(even, first, last)


def corner_kernel(col_even, col_odd, quality, phase, row_even, row_odd):
    rows = quality.shape[0]
    even, at_end = position("col")
    low = lax.broadcasted_iota(jnp.int32, (1, LANE), 1) < COL_HALO
    met = col_even[...]
    other = jnp.where(at_end, 0.0, col_odd[...])
    right = jnp.where(even, met, other)
    left = jnp.where(even, other, met)
    quality[...] = jnp.where(low, right, left)
    phase[...] = pltpu.roll(jnp.where(low, left, right), COL_HALO, 1)
    even, _ = position("row")
    bottom = rows - ROW_HALO
    for out, start in ((row_even, jnp.where(even, bottom, 0)), (row_odd, jnp.where(even, 0, bottom))):
        here = pl.ds(aligned(start), ROW_HALO)
        out[0:ROW_HALO, :] = quality[here, :]
        out[ROW_HALO : 2 * ROW_HALO, :] = phase[here, :]


class Stores:
    def __init__(self):
        self.waiting = []

    def put(self, ref, index, value):
        self.waiting.append((ref, index, value))

    def flush(self):
        for ref, index, value in self.waiting:
            ref[index] = value
        self.waiting = []


def run(count, step, carry, unroll):
    unroll = min(count, unroll)

    def turn(t, carry):
        stores = Stores()
        for u in range(unroll):
            carry = step(t * unroll + u, carry, stores.put)
        stores.flush()
        return carry

    turns = count // unroll
    if count <= WHOLE:
        for t in range(turns):
            carry = turn(t, carry)
    else:
        carry = lax.fori_loop(0, turns, turn, carry)
    assert turns * unroll == count
    return carry


def close(field, count):
    field[count] = chunk_below(field[0])


def put_level(put, level, i, *values):
    for key, value in zip(TOP_KEYS, values):
        put(level[key], i, value)


def spread(x, steps):
    return jnp.where((lane_index(x.shape[1]) & steps) != 0, x, right_of(x, steps))


def go_down(fine, coarse, depth, shape):
    steps = 1 << depth
    count = shape.slabs(depth + 1)
    a_f, b_f, gd_f, gr_f, v_f = (fine[k] for k in ("a", "b", "gd", "gr", "est"))
    last_level = depth + 1 == GRIDS

    def down_part(k):
        a = a_f[2 * k + 1]
        flux = gd_f[2 * k + 1] + a * (v_f[2 * k + 2] - v_f[2 * k + 1])
        return a + left_of(a, steps), flux + left_of(flux, steps)

    def step(k, carry, put):
        a_prev, gd_prev = carry
        a, gd = down_part(k)
        v0, v1 = v_f[2 * k], v_f[2 * k + 1]
        b0, b1 = b_f[2 * k], b_f[2 * k + 1]
        gr = gr_f[2 * k] + gr_f[2 * k + 1] + b0 * (right_of(v0, steps) - v0) + b1 * (right_of(v1, steps) - v1)
        b = b0 + b1
        right_side = gd - gd_prev + gr - left_of(gr, 2 * steps)
        if last_level:
            put(coarse["w"], k, a + b)
            put(coarse["est"], k, right_side)
        else:
            w = relax_weight(a + a_prev + b + left_of(b, 2 * steps))
            put_level(put, coarse, k, a, b, gd, gr, w, w * right_side)
        return a, gd

    a, gd = down_part(count - 1)
    run(count, step, (chunk_above(a), chunk_above(gd)), UNROLL_DOWN)
    if not last_level:
        close(coarse["est"], count)


def lane_select(shape):
    place = lax.broadcasted_iota(jnp.int32, (shape.cols, LANE), 0)
    target = lax.broadcasted_iota(jnp.int32, (shape.cols, LANE), 1)
    return (place == target * CELL + CELL - 1).astype(jnp.bfloat16)


def parts_of(x, count):
    parts = []
    for _ in range(count):
        part = x.astype(jnp.bfloat16)
        x = x - part.astype(jnp.float32)
        parts.append(part)
    return parts


def rows_of_parts(x, count):
    return jnp.concatenate(parts_of(x, count), axis=0)


def product(left, right, count):
    n = left.shape[0] // count
    out = None
    for p in range(count):
        wide = jnp.dot(left[0 : (count - p) * n], right[p], preferred_element_type=jnp.float32)
        for q in reversed(range(count - p)):
            piece = wide[q * n : (q + 1) * n]
            out = piece if out is None else out + piece
    return out


def select_product(x, one_hot, count):
    n = x.shape[0]
    out = jnp.dot(rows_of_parts(x, count), one_hot, preferred_element_type=jnp.float32)
    return sum(out[p * n : (p + 1) * n] for p in range(count))


def publish(coarse, pack, out, shape):
    per, chunks = shape.per_chunk, shape.crows // shape.per_chunk
    weights = sum(coarse["w"][j][:, : shape.cols] for j in range(per))
    fields = [coarse["est"][j][:, : shape.cols] for j in range(per)] + [weights]
    packed = select_product(jnp.concatenate(fields, axis=0), lane_select(shape), 3)
    sub = lax.broadcasted_iota(jnp.int32, (SUB, LANE), 0)
    total = jnp.sum(jnp.where(sub < chunks, packed[per * SUB :], 0.0), axis=0, keepdims=True)
    block = None
    for j in range(per):
        pack[j] = packed[j * SUB : (j + 1) * SUB]
    stride = shape.group // per
    for t in range(stride):
        for j in range(per):
            shift = (per * t + j) * shape.ccols
            x = pack[j, pl.ds(t, shape.block_rows, stride=stride), :]
            x = pltpu.roll(x, shift, 1) if shift else x
            block = x if block is None else block + x
    row = lax.broadcasted_iota(jnp.int32, block.shape, 0)
    block = jnp.where(row == shape.block_rows - 1, total, block)
    for device in range(shape.row_count * shape.col_count):
        out[device] = block


LEVEL_KEYS = ("a", "b", "gd", "gr", "w", "est")
TOP_KEYS = LEVEL_KEYS + ("bl", "gl")
LEVEL_REFS = len(TOP_KEYS) + (GRIDS - 1) * len(LEVEL_KEYS)


def levels_down(level0, levels, last, pack, out, shape):
    chain = [level0] + levels + [last]
    for depth in range(GRIDS):
        go_down(chain[depth], chain[depth + 1], depth, shape)
    publish(last, pack, out, shape)


def coarse_correction(gathered, tables, shape, corr):
    transforms, row_tables, inverse = tables
    rows, cols = shape.row_count, shape.col_count // shape.fold
    per, ccols, group = shape.per_chunk, shape.ccols, shape.group
    gr, gc = shape.grid_rows, shape.grid_cols
    lane = lane_index(LANE)
    blocks = []
    for g in range(group):
        for r in range(rows):
            pieces = []
            for tile in range(cols // group):
                piece = None
                for place in range(group):
                    x = gathered[r * cols + tile * group + place]
                    shift = ((place - g) * ccols) % LANE
                    x = pltpu.roll(x, shift, 1) if shift else x
                    piece = x if piece is None else jnp.where(lane >= place * ccols, x, piece)
                pieces.append(piece)
            blocks.append(jnp.concatenate(pieces, axis=1))
    strip = jnp.concatenate(blocks, axis=0)

    weights = gathered[0]
    for device in range(1, rows * cols):
        weights = weights + gathered[device]
    sub = lax.broadcasted_iota(jnp.int32, (SUB, LANE), 0)
    here = (sub % shape.block_rows == shape.block_rows - 1) & (lane < ccols)
    total = jnp.sum(jnp.where(here, weights, 0.0), keepdims=True)
    count = (gr - 1) * gc + gr * (gc - 1)
    mean = total / count + epsilon

    forward = 3 * shape.fold * gr
    spectrum = product(row_tables[0:forward, : strip.shape[0]], parts_of(strip, 3), 3)
    spectrum = jnp.concatenate([spectrum[f * gr : (f + 1) * gr] for f in range(shape.fold)], axis=1)
    spectrum = product(rows_of_parts(spectrum, 3), [transforms[p * gc : (p + 1) * gc] for p in range(3)], 3)
    spectrum = spectrum * (inverse[...] * (1.0 / mean))
    slots = SUB * per
    start = pl.multiple_of(forward + lax.axis_index("row") * 2 * slots, 2 * slots)
    backward = row_tables[pl.ds(start, 2 * slots), :][:, :gr]
    values = product(backward, parts_of(spectrum, 2), 2)
    values = product(rows_of_parts(values, 2), [transforms[p * gc : (p + 1) * gc] for p in (3, 4)], 2)

    def at(dim, size):
        return lax.broadcasted_iota(jnp.int32, size, dim)

    size = (gc, shape.lanes)
    cell = at(1, size) // CELL
    edge = (shape.cols + COL_HALO) // CELL
    cell = jnp.where(cell < edge, cell, cell - shape.lanes // CELL)
    to_lanes = (at(0, size) == cell + lax.axis_index("col") * ccols).astype(jnp.bfloat16)
    values = select_product(values, to_lanes, 2)
    for j in range(per):
        corr[j] = values[j * SUB : (j + 1) * SUB]
    close(corr, per)


def go_up(level, corr, depth, shape, emit):
    steps = 1 << depth
    count = shape.slabs(depth)
    a_r, b_r, gd_r, gr_r, w_r, e_r = (level[k] for k in LEVEL_KEYS)
    top = depth == 0

    def down_flux(i, v, v_next):
        return gd_r[i] + a_r[i] * (v_next - v)

    def sweep(i, v, v_next, f_prev, put):
        fd = down_flux(i, v, v_next)
        fr = gr_r[i] + b_r[i] * (right_of(v, steps) - v)
        fl = level["gl"][i] + level["bl"][i] * (v - left_of(v, 1)) if top else left_of(fr, steps)
        emit(put, i, v + w_r[i] * (fd - f_prev + fr - fl))
        return fd

    def pair(k, carry, put):
        v0, f_prev = carry
        v1 = e_r[2 * k + 1] + corr[k]
        v2 = e_r[2 * k + 2] + corr[k + 1]
        f_prev = sweep(2 * k, v0, v1, f_prev, put)
        return v2, sweep(2 * k + 1, v1, v2, f_prev, put)

    v_last = e_r[count - 1] + corr[count // 2 - 1]
    v_wrap = e_r[count] + corr[count // 2]
    f_prev = chunk_above(down_flux(count - 1, v_last, v_wrap))
    run(count // 2, pair, (e_r[0] + corr[0], f_prev), UNROLL_UP)


def levels_up(levels, corr, results, shape):
    for depth in range(GRIDS - 1, 0, -1):
        out = results[depth - 1]

        def emit(put, i, value, out=out, depth=depth):
            put(out, i, spread(value, 1 << (depth - 1)))

        go_up(levels[depth - 1], corr, depth, shape, emit)
        close(out, shape.slabs(depth))
        corr = out
    return corr


def as_levels(refs):
    n, top = len(LEVEL_KEYS), len(TOP_KEYS)
    rest = [dict(zip(LEVEL_KEYS, refs[i : i + n])) for i in range(top, len(refs), n)]
    return [dict(zip(TOP_KEYS, refs[:top]))] + rest


def start_kernel(*refs, shape):
    (quality, counts, row_even, row_odd, edge_q, edge_n, corner_even, corner_odd) = refs[:8]
    refs = refs[9:]
    out = refs[0]
    sd_r, sr_r, sl_r = refs[1:4]
    level_refs = refs[4 : 4 + LEVEL_REFS]
    nat_q, nat_n, q_r, n_r, rhs, wsum, pack = refs[4 + LEVEL_REFS :]
    rows, ext, tiles = shape.rows, shape.ext_rows, shape.tiles
    level0, *levels = as_levels(level_refs)

    even, at_end = position("row")
    below, above = rows, ext - ROW_HALO
    met = pl.ds(aligned(jnp.where(even, below, above)), ROW_HALO)
    other = pl.ds(aligned(jnp.where(even, above, below)), ROW_HALO)
    for t in range(tiles + 1):
        lanes = slice(t * LANE, (t + 1) * LANE) if t < tiles else slice(0, LANE)
        own_q, own_n, from_even, from_odd = (
            (quality, counts, row_even, row_odd) if t < tiles else (edge_q, edge_n, corner_even, corner_odd)
        )
        for nat, own, start in ((nat_q, own_q, 0), (nat_n, own_n, ROW_HALO)):
            nat[t, 0:rows, :] = own[:, lanes]
            nat[t, met, :] = from_even[start : start + ROW_HALO, lanes]
            nat[t, other, :] = jnp.where(at_end, 0.0, from_odd[start : start + ROW_HALO, lanes])
            if ext > rows + 2 * ROW_HALO:
                gap = slice(rows + ROW_HALO, ext - ROW_HALO)
                nat[t, gap, :] = jnp.zeros_like(nat[t, gap, :])
    count = shape.chunk

    def relay(i, carry, put):
        rows_of = pl.ds(i, SUB, stride=shape.chunk)
        put(q_r, i, jnp.concatenate([nat_q[t, rows_of, :] for t in range(tiles + 1)], axis=1))
        put(n_r, i, jnp.concatenate([nat_n[t, rows_of, :] for t in range(tiles + 1)], axis=1))
        return carry

    run(count, relay, 0, UNROLL_TOP)
    close(q_r, count)
    close(n_r, count)

    def down_part(i):
        a = jnp.minimum(q_r[i], q_r[i + 1])
        sd = wrap_steps(n_r[i + 1] - n_r[i])
        return a, sd, -(a * sd)

    def step(i, carry, put):
        a_prev, gd_prev = carry
        a, sd, gd = down_part(i)
        q, n = q_r[i], n_r[i]
        b, bl = jnp.minimum(q, right_of(q, 1)), jnp.minimum(q, left_of(q, 1))
        sr, sl = wrap_steps(right_of(n, 1) - n), wrap_steps(n - left_of(n, 1))
        gr, gl = -(b * sr), -(bl * sl)
        w = relax_weight(a + a_prev + b + bl)
        put_level(put, level0, i, a, b, gd, gr, w, w * (gd - gd_prev + gr - gl), bl, gl)
        put(sd_r, i, sd)
        put(sr_r, i, sr)
        put(sl_r, i, sl)
        return a, gd

    a, _, gd = down_part(count - 1)
    run(count, step, (chunk_above(a), chunk_above(gd)), UNROLL_TOP)
    close(level0["est"], count)
    levels_down(level0, levels, dict(est=rhs, w=wsum), pack, out, shape)


def middle_kernel(*refs, shape):
    gathered, tables, (sd_r, sr_r, sl_r) = refs[0], refs[1:4], refs[4:7]
    old = as_levels(refs[7 : 7 + LEVEL_REFS])
    refs = refs[7 + LEVEL_REFS :]
    out, first = refs[:2]
    level0, *levels = as_levels(refs[2 : 2 + LEVEL_REFS])
    rhs, wsum, pack, corr, *results = refs[2 + LEVEL_REFS :]
    coarse_correction(gathered, tables, shape, corr)
    field = levels_up(old[1:], corr, results, shape)

    def emit(put, i, value):
        put(first, i, value)

    count = shape.chunk
    go_up(old[0], field, 0, shape, emit)
    close(first, count)
    a_old, b_old, bl_old = (old[0][k] for k in ("a", "b", "bl"))

    def reweighted(weight, error):
        weight = weight / jnp.maximum(jnp.abs(error), error_floor)
        return weight, weight * error

    def down_part(i):
        return reweighted(a_old[i], first[i + 1] - first[i] - sd_r[i])

    def step(i, carry, put):
        a_prev, gd_prev = carry
        a, gd = down_part(i)
        v = first[i]
        b, gr = reweighted(b_old[i], right_of(v, 1) - v - sr_r[i])
        bl, gl = reweighted(bl_old[i], v - left_of(v, 1) - sl_r[i])
        w = relax_weight(a + a_prev + b + bl)
        put_level(put, level0, i, a, b, gd, gr, w, w * (gd - gd_prev + gr - gl), bl, gl)
        return a, gd

    a, gd = down_part(count - 1)
    run(count, step, (chunk_above(a), chunk_above(gd)), UNROLL_TOP)
    close(level0["est"], count)
    levels_down(level0, levels, dict(est=rhs, w=wsum), pack, out, shape)


def end_kernel(*refs, shape):
    gathered, tables, first = refs[0], refs[1:4], refs[4]
    old = as_levels(refs[5 : 5 + LEVEL_REFS])
    out, nat, corr, *results = refs[5 + LEVEL_REFS :]
    coarse_correction(gathered, tables, shape, corr)
    field = levels_up(old[1:], corr, results, shape)

    def emit(put, i, value):
        value = value + first[i]
        for t in range(shape.tiles):
            place = (t, pl.ds(i, SUB, stride=shape.chunk), slice(None))
            put(nat, place, value[:, t * LANE : (t + 1) * LANE])

    go_up(old[0], field, 0, shape, emit)
    for t in range(shape.tiles):
        out[:, t * LANE : (t + 1) * LANE] = nat[t, 0 : shape.rows, :]


def dct_table(count):
    freq = np.arange(count)[:, None]
    place = np.arange(count)[None, :]
    table = np.cos(np.pi * (((2 * place + 1) * freq) % (4 * count)) / (2 * count)) * np.sqrt(2.0 / count)
    table[0] *= np.sqrt(0.5)
    return table.astype(np.float32)


def in_parts(x, count):
    x = np.asarray(x, np.float32)
    parts = []
    for _ in range(count):
        part = x.astype(jnp.bfloat16)
        x = x - part.astype(np.float32)
        parts.append(part)
    return np.concatenate(parts, axis=0)


def solve_tables(shape):
    gr, gc, per, crows, ccols = shape.grid_rows, shape.grid_cols, shape.per_chunk, shape.crows, shape.ccols
    fold, group, height = shape.fold, shape.group, shape.block_rows
    table_x, table_y = dct_table(gr), dct_table(gc)
    g, r, f, q = (
        x.ravel()
        for x in np.meshgrid(*map(np.arange, (group, shape.row_count, fold, height)), indexing="ij")
    )
    local = group * q + g
    inside = local < crows
    rows = table_x[:, np.where(inside, r * crows + local, 0)]
    forward = np.concatenate([np.where(inside & (f == n), rows, 0) for n in range(fold)], axis=0)
    f, c, j = (
        x.ravel() for x in np.meshgrid(*map(np.arange, (fold, shape.col_count // fold, ccols)), indexing="ij")
    )
    columns = table_y[:, (c * fold + f) * ccols + j].T
    slab, chunk = (x.ravel() for x in np.meshgrid(np.arange(per), np.arange(SUB), indexing="ij"))
    local = chunk * per + slab
    slots = SUB * per
    local = np.where(local < slots - ROW_HALO // CELL, local, local - slots)
    backward = [table_x.T[np.clip(r * crows + local, 0, gr - 1)] for r in range(shape.row_count)]
    width = -(-max(forward.shape[1], gr) // LANE) * LANE
    row_tables = [in_parts(forward, 3)] + [in_parts(x, 2) for x in backward]
    row_tables = np.concatenate([np.pad(x, ((0, 0), (0, width - x.shape[1]))) for x in row_tables], axis=0)
    transforms = np.concatenate([in_parts(columns, 3), in_parts(table_y, 2)], axis=0)
    lam_x = 2 - 2 * np.cos(np.pi * np.arange(gr) / gr)
    lam_y = 2 - 2 * np.cos(np.pi * np.arange(gc) / gc)
    inverse = 1 / (lam_x[:, None] + lam_y[None, :] + (screen_width / gc) ** 2)
    return [jnp.asarray(transforms), jnp.asarray(row_tables), jnp.asarray(inverse, jnp.float32)]


def f32(*dims):
    return jax.ShapeDtypeStruct(dims, jnp.float32)


def level_shapes(shape):
    return [
        f32(shape.slabs(d) + (key == "est"), SUB, shape.lanes)
        for d in range(GRIDS)
        for key in (LEVEL_KEYS if d else TOP_KEYS)
    ]


def vmem(*dims):
    return pltpu.VMEM(dims, jnp.float32)


def swap(even_strip, odd_strip, axis):
    rows, cols = lax.axis_size("row"), lax.axis_size("col")
    even_pairs, odd_pairs = [], []
    for r in range(rows):
        for c in range(cols):
            here = r * cols + c
            index, count, step = (r, rows, cols) if axis == "row" else (c, cols, 1)
            even_pairs.append((here, here + step * ((index ^ 1) - index)))
            if 0 < index < count - 1:
                odd_pairs.append((here, here + (step if index % 2 else -step)))
            else:
                odd_pairs.append((here, idle_pair(axis, r, c, rows, cols)))
    both = ("row", "col")
    return lax.ppermute(even_strip, both, even_pairs), lax.ppermute(odd_strip, both, odd_pairs)


def idle_pair(axis, r, c, rows, cols):
    if axis == "col":
        return (r ^ 1) * cols + c
    return (rows - 1 - r) * cols + c


def gather(blocks):
    blocks = lax.all_to_all(blocks, ("row", "col"), split_axis=0, concat_axis=0, tiled=True)
    return blocks.reshape(-1, SUB, LANE)


def body(swath, coherence, phase_counts, *, shape):
    params = pltpu.CompilerParams(vmem_limit_bytes=16 * 2**20)
    rows, cols = shape.rows, shape.cols
    block = f32(shape.row_count * shape.col_count, shape.block_rows, LANE)
    tables = solve_tables(shape)
    coarse_scratch = [vmem(shape.per_chunk, SUB, shape.lanes)] * 2 + [vmem(shape.per_chunk, SUB, LANE)]
    result_scratch = [vmem(shape.per_chunk + 1, SUB, shape.lanes)]
    result_scratch += [vmem(shape.slabs(d) + 1, SUB, shape.lanes) for d in range(1, GRIDS)]

    strip, edge, corner = f32(2 * ROW_HALO, cols), f32(rows, LANE), f32(2 * ROW_HALO, LANE)
    quality, counts, row_even, row_odd, col_even, col_odd = pl.pallas_call(
        strips_kernel,
        in_specs=[pl.BlockSpec(memory_space=pltpu.HBM)] * 3,
        out_shape=[f32(rows, cols), f32(rows, cols), strip, strip, edge, edge],
        scratch_shapes=[pltpu.VMEM((rows, cols), jnp.int32)] * 3 + [pltpu.SemaphoreType.DMA((3,))],
        compiler_params=params,
        name="strips",
    )(*(pltpu.with_memory_space_constraint(x, pltpu.HBM) for x in (swath, coherence, phase_counts)))
    row_even, row_odd = swap(row_even, row_odd, "row")
    col_even, col_odd = swap(col_even, col_odd, "col")
    edge_q, edge_n, corner_even, corner_odd = pl.pallas_call(
        corner_kernel,
        out_shape=[edge, edge, corner, corner],
        compiler_params=params,
        name="corners",
    )(col_even, col_odd)
    corner_even, corner_odd = swap(corner_even, corner_odd, "row")

    slabs = (shape.chunk, SUB, shape.lanes)
    more = (shape.chunk + 1, SUB, shape.lanes)
    nat = vmem(shape.tiles, shape.ext_rows, LANE)
    wide = vmem(shape.tiles + 1, shape.ext_rows, LANE)
    block_out, sd, sr, sl, *old = pl.pallas_call(
        functools.partial(start_kernel, shape=shape),
        out_shape=[block] + [f32(*slabs)] * 3 + level_shapes(shape),
        scratch_shapes=[wide, wide, vmem(*more), vmem(*more)] + coarse_scratch,
        compiler_params=params,
        name="start",
    )(quality, counts, row_even, row_odd, edge_q, edge_n, corner_even, corner_odd, tables[2])
    gathered = gather(block_out)
    block_out, first, *old = pl.pallas_call(
        functools.partial(middle_kernel, shape=shape),
        out_shape=[block, f32(*more)] + level_shapes(shape),
        scratch_shapes=coarse_scratch + result_scratch,
        compiler_params=params,
        name="middle",
    )(gathered, *tables, sd, sr, sl, *old)
    gathered = gather(block_out)
    return pl.pallas_call(
        functools.partial(end_kernel, shape=shape),
        out_shape=f32(rows, cols),
        scratch_shapes=[nat] + result_scratch,
        compiler_params=params,
        name="finish",
    )(gathered, *tables, first, *old)


def solution(mesh):
    def run(swath, coherence, phase_counts):
        rows, cols = swath.shape
        row_count, col_count = mesh.shape["row"], mesh.shape["col"]
        shape = Shape(rows // row_count, cols // col_count, row_count, col_count)
        return jax.shard_map(
            functools.partial(body, shape=shape),
            mesh=mesh,
            in_specs=(P("row", "col"), P("row", "col"), P("row", "col")),
            out_specs=P("row", "col"),
            check_vma=False,
        )(swath, coherence, phase_counts)

    return run
```
